32 devices in a mesh: gx: 4 (over y, core), gy: 2 (over x), var: 4 (over z).
Axes of the slice: x: 2, y: 2, z: 4, core: 2. Of those that a mesh axis runs over, the one named last changes fastest.
Arguments:
- field: float32 [4, 32, 256, 256], P('var', None, 'gx', 'gy'), may hold values from -12 to 12
- drive: float32 [4, 32, 40, 40], P('var'), may hold values from -1 to 1
- keep_count: int32 [32], replicated, may hold values from 20 to 79, as said below
- level_class: int32 [32], replicated, may hold values from 0 to 7
- height_table: float32 [8], replicated, may hold values from 0.2 to 1
Outputs:
- nudged: float32 [4, 32, 256, 256], P('var', None, 'gx', 'gy')
The draws below stay inside these ranges and needn't reach their ends.
Inputs may be any that keep to these rules, and one draw needn't show every extreme that they name: `keep_count`: some level in every draw has the count 2 * 40 - 1, which keeps all 40 x 40 modes.
All inputs are finite; a program needn't handle non-finite values.
Results may differ from the reference program's by a relative error of at most 0.0001.
Values sent between devices are 32-bit elements; how exact they have to be, the bound alone decides.
No kernel may reach another device: no remote copies, remote signals or barrier semaphores. Data moves between devices by JAX's collectives and lax.ppermute only.
A program may use at most 64 MiB of HBM per device.

```python
import math
import jax
import jax.numpy as jnp
from jax import lax

NVAR = 4
KM = 40
HTAB = 8
LEVELS = 32
NX = 256
NY = 256


def cosine_table_drawn(first, count, total, modes):
    cells = first + jnp.arange(count, dtype=jnp.int32)
    waves = jnp.arange(modes, dtype=jnp.int32)
    phase = waves[None, :] * (2 * cells[:, None] + 1) % (4 * total)
    values = jnp.cos(jnp.pi * phase.astype(jnp.float32) / (2.0 * total))
    factor = jnp.where(waves == 0, 1.0, math.sqrt(2.0)).astype(jnp.float32)
    return values * factor[None, :]


def draw_field(key, part):
    key_amp, key_rough = jax.random.split(jax.random.fold_in(key, 11), 2)
    waves = jnp.arange(KM, dtype=jnp.int32)
    damping = 0.25 / (1.0 + (waves[:, None] + waves[None, :]).astype(jnp.float32) / 8.0)
    amplitude = jax.random.normal(key_amp, (NVAR, LEVELS, KM, KM), jnp.float32) * damping
    table_x = cosine_table_drawn(0, NX, NX, KM)
    table_y = cosine_table_drawn(0, NY, NY, KM)
    back = jnp.einsum('vlmn,jn->vlmj', amplitude, table_y)
    smooth = jnp.einsum('vlmj,im->vlij', back, table_x)
    rough = jax.random.normal(key_rough, (NVAR, LEVELS, NX, NY), jnp.float32)
    return jnp.clip(smooth + rough, -12.0, 12.0)


def draw_keep_count(key, part):
    key_counts, key_level = jax.random.split(jax.random.fold_in(key, 23), 2)
    counts = jax.random.randint(key_counts, (LEVELS,), KM // 2, 2 * KM - 1, dtype=jnp.int32)
    chosen = jax.random.randint(key_level, (), 0, LEVELS, dtype=jnp.int32)
    return jnp.where(jnp.arange(LEVELS, dtype=jnp.int32) == chosen, 2 * KM - 1, counts).astype(jnp.int32)


def place_ends(result, key, smallest, top_value):
    extent = result.shape
    index_at = [jax.random.randint(jax.random.fold_in(key, axis), (), 0, extent[axis]) for axis in range(len(extent))]
    result = result.at[tuple(index_at)].set(smallest)
    longest = extent.index(max(extent))
    index_at[longest] = (index_at[longest] + 1) % extent[longest]
    return result.at[tuple(index_at)].set(top_value)


def block_levels(key, shape, cuts, smallest, largest):
    def one(position, shards_of):
        steps = jax.random.uniform(jax.random.fold_in(jax.random.fold_in(key, 6), position), (shards_of,), jnp.float32, smallest / len(cuts), largest / len(cuts))
        return jnp.repeat(jnp.exp(steps), shape[position] // shards_of).reshape((-1,) + (1,) * (len(shape) - position - 1))

    level = one(*cuts[0])
    for cut in cuts[1:]:
        level = level * one(*cut)
    return level


def bell_draw(rng, extent, scale, most, shards=(), held_as=jnp.bfloat16):
    values = scale * jax.random.normal(rng, extent, jnp.float32)
    if shards:
        values = values * block_levels(rng, extent, shards, -0.22, 0.18)
    return jnp.clip(values, -most, most).astype(held_as)


def setup_inputs(seed: int = 0) -> dict:
    streams_of = jax.random.split(jax.random.key(seed), 6)
    return {
        "field": draw_field(jax.random.fold_in(streams_of[5], 71), 0),
        "drive": bell_draw(streams_of[1], (NVAR, LEVELS, KM, KM), 0.15, 1.0, ((0, 4),), jnp.float32),
        "keep_count": draw_keep_count(jax.random.fold_in(streams_of[5], 71), 0),
        "level_class": place_ends(jax.random.randint(streams_of[3], (LEVELS,), 0, HTAB), jax.random.fold_in(streams_of[3], 1), 0, HTAB - 1).astype(jnp.int32),
        "height_table": jnp.clip(jnp.exp(jax.random.uniform(streams_of[4], (HTAB,), jnp.float32, math.log(0.2), math.log(1.0))), 0.2, 1.0),
    }


energy_weights = (1.0, 1.0, 2.0, 3.0)
strength_top = 0.5
epsilon = 1e-06

def cosine_table(first, count, total, modes):
    cells = first + jnp.arange(count, dtype=jnp.int32)
    waves = jnp.arange(modes, dtype=jnp.int32)
    phase = waves[None, :] * (2 * cells[:, None] + 1) % (4 * total)
    values = jnp.cos(jnp.pi * phase.astype(jnp.float32) / (2.0 * total))
    factor = jnp.where(waves == 0, 1.0, math.sqrt(2.0)).astype(jnp.float32)
    return values * factor[None, :]

def reference(field, drive, keep_count, level_class, height_table):
    high = lax.Precision.HIGHEST
    table_x = cosine_table(0, NX, NX, KM)
    table_y = cosine_table(0, NY, NY, KM)
    waves = jnp.arange(KM, dtype=jnp.int32)
    mask = ((waves[:, None] + waves[None, :])[None, :, :] < keep_count[:, None, None]).astype(jnp.float32)
    onehot = (level_class[:, None] == jnp.arange(HTAB, dtype=jnp.int32)[None, :]).astype(jnp.float32)
    lift = jnp.dot(onehot, height_table, precision=high)
    band_gap = jnp.zeros((), jnp.float32)
    band_model = jnp.zeros((), jnp.float32)
    deltas = []
    for index in range(NVAR):
        half = jnp.einsum('lij,im->lmj', field[index], table_x, precision=high)
        coeff = jnp.einsum('lmj,jn->lmn', half, table_y, precision=high) / float(NX * NY)
        delta = mask * (drive[index] - coeff)
        band_gap = band_gap + energy_weights[index] * jnp.sum(delta * delta)
        band_model = band_model + energy_weights[index] * jnp.sum(mask * coeff * coeff)
        deltas.append(delta)
    strength = strength_top * band_gap / (band_gap + band_model + epsilon)
    results = []
    for index in range(NVAR):
        back = jnp.einsum('lmn,jn->lmj', deltas[index], table_y, precision=high)
        increment = jnp.einsum('lmj,im->lij', back, table_x, precision=high)
        results.append(field[index] + strength * lift[:, None, None] * increment)
    return jnp.stack(results)
```

```python
import numpy as np

import jax
import jax.numpy as jnp
from jax import lax
from jax.experimental import pallas as pl
from jax.experimental.pallas import tpu as pltpu
from jax.sharding import PartitionSpec as P

energy_weights = (1.0, 1.0, 2.0, 3.0)
strength_top = 0.5
epsilon = 1e-06


LANES = 128
HIGH = lax.Precision.HIGHEST
VMEM = pltpu.MemorySpace.VMEM
SMEM = pltpu.MemorySpace.SMEM


def cosine_table(total, modes):
    cells = np.arange(total, dtype=np.int64)
    waves = np.arange(modes, dtype=np.int64)
    phase = waves[None, :] * (2 * cells[:, None] + 1) % (4 * total)
    factor = np.where(waves == 0, 1.0, np.sqrt(2.0))
    return (np.cos(np.pi * phase / (2.0 * total)) * factor[None, :]).astype(np.float32)


def dot(a, b):
    return jnp.dot(a, b, precision=HIGH, preferred_element_type=jnp.float32)


def pack_lanes(pieces, modes):
    tiles = -(-len(pieces) * modes // LANES)
    out = [None] * tiles
    lane = lax.broadcasted_iota(jnp.int32, pieces[0].shape, 1)

    def put(tile, value):
        out[tile] = value if out[tile] is None else out[tile] + value

    for index, piece in enumerate(pieces):
        tile, offset = divmod(index * modes, LANES)
        turned = pltpu.roll(piece, offset, 1) if offset else piece
        if offset + modes > LANES:
            put(tile, jnp.where(lane >= offset, turned, 0.0))
            put(tile + 1, jnp.where(lane < offset, turned, 0.0))
        else:
            put(tile, turned)
    return out


def unpack_lanes(tiles, count, modes):
    lane = lax.broadcasted_iota(jnp.int32, tiles[0].shape, 1)
    pieces = []
    for index in range(count):
        tile, offset = divmod(index * modes, LANES)
        piece = tiles[tile]
        if offset + modes > LANES:
            piece = jnp.where(lane >= offset, piece, tiles[tile + 1])
        pieces.append(pltpu.roll(piece, LANES - offset, 1) if offset else piece)
    return pieces


def forward_kernel(core_ref, block_ref, tx_ref, ty_ref, keep_ref, send_ref):
    levels = block_ref.shape[0]
    half = levels // 2
    modes = tx_ref.shape[0]
    core = core_ref[0]
    tx = tx_ref[...]
    ty = ty_ref[...]
    for out_ref, first in ((send_ref, (1 - core) * half), (keep_ref, core * half)):
        wide = jnp.concatenate([block_ref[first + l] for l in range(half)], axis=1)
        part = dot(tx, wide)
        tall = jnp.concatenate([part[:, l * LANES : (l + 1) * LANES] for l in range(half)], axis=0)
        coeff = dot(tall, ty)
        tiles = pack_lanes([coeff[l * modes : (l + 1) * modes] for l in range(half)], modes)
        for t, tile in enumerate(tiles):
            out_ref[:, t * LANES : (t + 1) * LANES] = tile


def settle_kernel(core_ref, weight_ref, keep_count_ref, own_ref, *rest):
    *others, drive_ref, delta_ref, energy_ref = rest
    modes, width = own_ref.shape
    half = width // modes
    core = core_ref[0]
    weight = weight_ref[0]
    lane = lax.broadcasted_iota(jnp.int32, (8, LANES), 1)
    row = lax.broadcasted_iota(jnp.int32, (8, LANES), 0)
    gap = jnp.zeros((8, LANES), jnp.float32)
    model = jnp.zeros((8, LANES), jnp.float32)
    pad = jnp.zeros((modes, LANES - modes), jnp.float32)
    drive = pack_lanes(
        [jnp.concatenate([drive_ref[core * half + l], pad], axis=1) for l in range(half)], modes
    )
    for t in range(width // LANES):
        level = (lane + t * LANES) // modes
        wave = (lane + t * LANES) - level * modes
        keep = jnp.zeros((8, LANES), jnp.int32)
        for l in range(t * LANES // modes, min(half, ((t + 1) * LANES - 1) // modes + 1)):
            keep = jnp.where(level == l, keep_count_ref[core * half + l], keep)
        for r in range(0, modes, 8):
            at = (slice(r, r + 8), slice(t * LANES, (t + 1) * LANES))
            coeff = own_ref[at]
            for other in others:
                coeff = coeff + other[at]
            mask = (row + r + wave < keep).astype(jnp.float32)
            delta = mask * (drive[t][r : r + 8] - coeff)
            delta_ref[at] = delta
            gap = gap + delta * delta
            model = model + mask * coeff * coeff
    energy_ref[0:8, :] = weight * gap
    energy_ref[8:16, :] = weight * model


def inverse_kernel(core_ref, class_ref, height_ref, own_ref, other_ref, tx_ref, ty_ref, out_ref):
    levels = out_ref.shape[0]
    half = levels // 2
    modes, width = own_ref.shape
    core = core_ref[0]
    tx = tx_ref[...]
    ty = ty_ref[...]
    for ref, first in ((own_ref, core * half), (other_ref, (1 - core) * half)):
        tiles = [ref[:, t * LANES : (t + 1) * LANES] for t in range(width // LANES)]
        tall = jnp.concatenate(unpack_lanes(tiles, half, modes), axis=0)
        back = dot(tall, ty)
        wide = jnp.concatenate([back[l * modes : (l + 1) * modes] for l in range(half)], axis=1)
        increment = dot(tx, wide)
        for l in range(half):
            lift = height_ref[class_ref[first + l]]
            out_ref[first + l] = lift * increment[:, l * LANES : (l + 1) * LANES]


def call(kernel, out_shape, spaces, name):
    return pl.pallas_call(
        kernel,
        out_shape=out_shape,
        in_specs=[pl.BlockSpec(memory_space=s) for s in spaces],
        out_specs=jax.tree.map(lambda _: pl.BlockSpec(memory_space=VMEM), out_shape),
        name=name,
    )


def solution(mesh):
    count_x, count_y, count_v = (mesh.shape[a] for a in ("gx", "gy", "var"))
    ranks = count_x * count_y
    for count in (count_x, count_y, count_v):
        assert count & (count - 1) == 0

    def swap(value, bits):
        return lax.ppermute(value, ("gx", "gy"), [(i, i ^ bits) for i in range(ranks)])

    bits_x = [count_y << b for b in range(1, count_x.bit_length() - 1)]
    bits_y = [1 << b for b in range(count_y.bit_length() - 1)]
    stages = []
    for b in range(max(len(bits_x), len(bits_y))):
        bx, by = bits_x[b : b + 1], bits_y[b : b + 1]
        stages.append(bx + by + [x | y for x in bx for y in by])

    def per_device(field, drive, keep_count, level_class, height_table):
        block = field[0]
        levels, rows, columns = block.shape
        modes = drive.shape[-1]
        half = levels // 2
        total_x, total_y = rows * count_x, columns * count_y
        assert columns == LANES and levels % 2 == 0 and half * modes % LANES == 0 and modes % 8 == 0
        table_x = cosine_table(total_x, modes).reshape(count_x, rows, modes)
        table_y = cosine_table(total_y, modes).reshape(count_y, columns, modes)
        wide_y = np.zeros((count_y, columns, LANES), np.float32)
        wide_y[:, :, :modes] = table_y
        at_x, at_y = lax.axis_index("gx"), lax.axis_index("gy")
        pick = lambda table, at: lax.dynamic_index_in_dim(jnp.asarray(table), at, 0, False)
        tx = pick(table_x, at_x)
        tx_t = pick(table_x.transpose(0, 2, 1) / np.float32(total_x * total_y), at_x)
        ty = pick(wide_y, at_y)
        ty_t = pick(wide_y.transpose(0, 2, 1), at_y)
        core = (at_x % 2).reshape(1)
        weight = jnp.asarray(energy_weights, jnp.float32)[lax.axis_index("var")].reshape(1)
        shape = jax.ShapeDtypeStruct((modes, half * modes), jnp.float32)

        keep, send = call(forward_kernel, (shape, shape), (SMEM, VMEM, VMEM, VMEM), "forward")(
            core, block, tx_t, ty
        )
        total = keep + swap(send, count_y)
        parts = [total]
        for stage in stages:
            if len(parts) > 1:
                parts = [sum(parts[1:], parts[0])]
            parts = parts + [swap(parts[0], bits) for bits in stage]
        delta, energy = call(
            settle_kernel,
            (shape, jax.ShapeDtypeStruct((16, LANES), jnp.float32)),
            (SMEM, SMEM, SMEM) + (VMEM,) * (len(parts) + 1),
            "settle",
        )(core, weight, keep_count, *parts, drive[0])
        energy = energy + swap(energy, count_y)
        other = swap(delta, count_y)
        for b in range(count_v.bit_length() - 1):
            energy = energy + lax.ppermute(energy, "var", [(i, i ^ (1 << b)) for i in range(count_v)])
        increment = call(
            inverse_kernel,
            jax.ShapeDtypeStruct(block.shape, jnp.float32),
            (SMEM, SMEM, SMEM) + (VMEM,) * 4,
            "inverse",
        )(core, level_class, height_table, delta, other, tx, ty_t)
        gap, model = jnp.sum(energy[:8]), jnp.sum(energy[8:])
        strength = strength_top * gap / (gap + model + epsilon)
        return (block + strength * increment)[None]

    return jax.shard_map(
        per_device,
        mesh=mesh,
        in_specs=(P("var", None, "gx", "gy"), P("var", None, None, None), P(), P(), P()),
        out_specs=P("var", None, "gx", "gy"),
        check_vma=False,
    )
```

```python
import numpy as np

import jax
import jax.numpy as jnp
from jax import lax
from jax.experimental import pallas as pl
from jax.experimental.pallas import tpu as pltpu
from jax.sharding import PartitionSpec as P

energy_weights = (1.0, 1.0, 2.0, 3.0)
strength_top = 0.5
epsilon = 1e-06


LANES = 128
HIGH = lax.Precision.HIGHEST
VMEM = pltpu.MemorySpace.VMEM
SMEM = pltpu.MemorySpace.SMEM
HBM = pltpu.MemorySpace.HBM


def cosine_table(total, modes):
    cells = np.arange(total, dtype=np.int64)
    waves = np.arange(modes, dtype=np.int64)
    phase = waves[None, :] * (2 * cells[:, None] + 1) % (4 * total)
    factor = np.where(waves == 0, 1.0, np.sqrt(2.0))
    return (np.cos(np.pi * phase / (2.0 * total)) * factor[None, :]).astype(np.float32)


def dot(a, b):
    return jnp.dot(a, b, precision=HIGH, preferred_element_type=jnp.float32)


def pack_lanes(pieces, modes):
    tiles = -(-len(pieces) * modes // LANES)
    out = [None] * tiles
    lane = lax.broadcasted_iota(jnp.int32, pieces[0].shape, 1)

    def put(tile, value):
        out[tile] = value if out[tile] is None else out[tile] + value

    for index, piece in enumerate(pieces):
        tile, offset = divmod(index * modes, LANES)
        turned = pltpu.roll(piece, offset, 1) if offset else piece
        if offset + modes > LANES:
            put(tile, jnp.where(lane >= offset, turned, 0.0))
            put(tile + 1, jnp.where(lane < offset, turned, 0.0))
        else:
            put(tile, turned)
    return out


def unpack_lanes(tiles, count, modes):
    lane = lax.broadcasted_iota(jnp.int32, tiles[0].shape, 1)
    pieces = []
    for index in range(count):
        tile, offset = divmod(index * modes, LANES)
        piece = tiles[tile]
        if offset + modes > LANES:
            piece = jnp.where(lane >= offset, piece, tiles[tile + 1])
        pieces.append(pltpu.roll(piece, LANES - offset, 1) if offset else piece)
    return pieces


def forward_kernel(field_ref, tx_ref, ty_ref, block_ref, keep_ref, send_ref, tx, ty, sems):
    levels = block_ref.shape[0]
    half = levels // 2
    modes = tx_ref.shape[1]
    at_x, at_y = lax.axis_index("gx"), lax.axis_index("gy")
    core = lax.rem(at_x, 2)
    firsts = ((1 - core) * half, core * half)

    def chunk(h, q):
        rows = pl.ds(firsts[h] + q * (half // 2), half // 2)
        return pltpu.make_async_copy(field_ref.at[0, rows], block_ref.at[rows], sems.at[2 * h + q])

    copies = [chunk(h, q) for h in range(2) for q in range(2)]
    tables = [
        pltpu.make_async_copy(tx_ref.at[at_x], tx, sems.at[4]),
        pltpu.make_async_copy(ty_ref.at[at_y], ty, sems.at[5]),
    ]
    for copy in tables + copies:
        copy.start()
    for copy in tables:
        copy.wait()
    for h, out_ref in enumerate((send_ref, keep_ref)):
        pieces = []
        for q in range(2):
            copies[2 * h + q].wait()
            first = firsts[h] + q * (half // 2)
            wide = jnp.concatenate([block_ref[first + l] for l in range(half // 2)], axis=1)
            part = dot(tx[...], wide)
            tall = jnp.concatenate(
                [part[:, l * LANES : (l + 1) * LANES] for l in range(half // 2)], axis=0
            )
            coeff = dot(tall, ty[...])
            pieces += [coeff[l * modes : (l + 1) * modes] for l in range(half // 2)]
        for t, tile in enumerate(pack_lanes(pieces, modes)):
            out_ref[:, t * LANES : (t + 1) * LANES] = tile


def prepare_kernel(
    _,
    keep_count_ref,
    class_ref,
    height_ref,
    drive_ref,
    tx_ref,
    ty_ref,
    goal_ref,
    mask_ref,
    lift_ref,
    tx_out_ref,
    ty_out_ref,
    drive,
    sems,
):
    half, modes, _ = drive.shape
    width = goal_ref.shape[1]
    at_x, at_y = lax.axis_index("gx"), lax.axis_index("gy")
    first = lax.rem(at_x, 2) * half
    copies = [
        pltpu.make_async_copy(drive_ref.at[0, pl.ds(first, half)], drive, sems.at[0]),
        pltpu.make_async_copy(tx_ref.at[at_x], tx_out_ref, sems.at[1]),
        pltpu.make_async_copy(ty_ref.at[at_y], ty_out_ref, sems.at[2]),
    ]
    for copy in copies:
        copy.start()
    for l in range(lift_ref.shape[0]):
        lift_ref[l : l + 1, :] = jnp.full((1, LANES), height_ref[class_ref[l]], jnp.float32)
    lane = lax.broadcasted_iota(jnp.int32, (8, LANES), 1)
    row = lax.broadcasted_iota(jnp.int32, (8, LANES), 0)
    for t in range(width // LANES):
        limit = jnp.zeros((8, LANES), jnp.int32)
        for l in range(t * LANES // modes, min(half, ((t + 1) * LANES - 1) // modes + 1)):
            wave = lane + (t * LANES - l * modes)
            limit = jnp.where(wave >= 0, keep_count_ref[first + l] - wave, limit)
        for r in range(0, modes, 8):
            mask_ref[r : r + 8, t * LANES : (t + 1) * LANES] = (row + r < limit).astype(jnp.float32)
    copies[0].wait()
    pad = jnp.zeros((modes, LANES - modes), jnp.float32)
    goal = pack_lanes([jnp.concatenate([drive[l], pad], axis=1) for l in range(half)], modes)
    for t, tile in enumerate(goal):
        goal_ref[:, t * LANES : (t + 1) * LANES] = tile
    for copy in copies[1:]:
        copy.wait()


def settle_kernel(goal_ref, mask_ref, own_ref, *rest):
    *others, delta_ref, energy_ref = rest
    modes, width = own_ref.shape
    variable = lax.axis_index("var")
    weight = jnp.float32(0.0)
    for index, value in enumerate(energy_weights):
        weight = jnp.where(variable == index, jnp.float32(value), weight)
    gap = jnp.zeros((8, LANES), jnp.float32)
    model = jnp.zeros((8, LANES), jnp.float32)
    for t in range(width // LANES):
        for r in range(0, modes, 8):
            at = (slice(r, r + 8), slice(t * LANES, (t + 1) * LANES))
            coeff = own_ref[at]
            for other in others:
                coeff = coeff + other[at]
            mask = mask_ref[at]
            delta = mask * (goal_ref[at] - coeff)
            delta_ref[at] = delta
            gap = gap + delta * delta
            model = model + mask * coeff * coeff
    energy_ref[0:8, :] = weight * gap
    energy_ref[8:16, :] = weight * model


def inverse_kernel(own_ref, other_ref, lift_ref, tx_ref, ty_ref, out_ref):
    levels = out_ref.shape[0]
    half = levels // 2
    modes, width = own_ref.shape
    core = lax.rem(lax.axis_index("gx"), 2)
    for ref, first in ((own_ref, core * half), (other_ref, (1 - core) * half)):
        tiles = [ref[:, t * LANES : (t + 1) * LANES] for t in range(width // LANES)]
        tall = jnp.concatenate(unpack_lanes(tiles, half, modes), axis=0)
        back = dot(tall, ty_ref[...])
        wide = jnp.concatenate([back[l * modes : (l + 1) * modes] for l in range(half)], axis=1)
        increment = dot(tx_ref[...], wide)
        for l in range(half):
            lift = lift_ref[pl.ds(first + l, 1), :]
            out_ref[first + l] = lift * increment[:, l * LANES : (l + 1) * LANES]


def finish_kernel(energy_ref, other_ref, block_ref, increment_ref, out_ref, buffer, sems):
    levels = block_ref.shape[0]
    energy = energy_ref[...] + other_ref[...]
    gap = jnp.sum(energy[:8], keepdims=True)
    model = jnp.sum(energy[8:], keepdims=True)
    strength = strength_top * gap / (gap + model + epsilon)
    count = sems.shape[0]
    copies = []
    for q in range(count):
        rows = pl.ds(q * (levels // count), levels // count)
        for l in range(q * (levels // count), (q + 1) * (levels // count)):
            buffer[l] = block_ref[l] + strength * increment_ref[l]
        copies.append(pltpu.make_async_copy(buffer.at[rows], out_ref.at[0, rows], sems.at[q]))
        copies[-1].start()
    for copy in copies:
        copy.wait()


def call(kernel, name, ins, outs, scratch=(), flops=0):
    return pl.pallas_call(
        kernel,
        out_shape=outs,
        in_specs=[pl.BlockSpec(memory_space=pl.ANY if s is HBM else s) for _, s in ins],
        out_specs=jax.tree.map(
            lambda o: pl.BlockSpec(memory_space=VMEM if isinstance(o, pl.MemoryRef) else pl.ANY),
            outs,
            is_leaf=lambda o: isinstance(o, (pl.MemoryRef, jax.ShapeDtypeStruct)),
        ),
        scratch_shapes=scratch,
        cost_estimate=pl.CostEstimate(flops=flops, transcendentals=0, bytes_accessed=0),
        name=name,
    )(*[pltpu.with_memory_space_constraint(x, VMEM) if s is VMEM else x for x, s in ins])


def solution(mesh):
    count_x, count_y, count_v = (mesh.shape[a] for a in ("gx", "gy", "var"))
    ranks = count_x * count_y
    for count in (count_x, count_y, count_v):
        assert count & (count - 1) == 0

    def swap(value, bits):
        return lax.ppermute(value, ("gx", "gy"), [(i, i ^ bits) for i in range(ranks)])

    def swap_var(value, bits):
        return lax.ppermute(value, "var", [(i, i ^ bits) for i in range(count_v)])

    bits_x = [count_y << b for b in range(1, count_x.bit_length() - 1)]
    bits_y = [1 << b for b in range(count_y.bit_length() - 1)]
    stages = []
    for b in range(max(len(bits_x), len(bits_y))):
        bx, by = bits_x[b : b + 1], bits_y[b : b + 1]
        stages.append(bx + by + [x | y for x in bx for y in by])

    def per_device(field, drive, keep_count, level_class, height_table):
        _, levels, rows, columns = field.shape
        modes = drive.shape[-1]
        half = levels // 2
        total_x, total_y = rows * count_x, columns * count_y
        assert columns == LANES and levels % 4 == 0 and half * modes % LANES == 0 and modes % 8 == 0
        table_x = cosine_table(total_x, modes).reshape(count_x, rows, modes)
        table_y = np.zeros((count_y, columns, LANES), np.float32)
        table_y[:, :, :modes] = cosine_table(total_y, modes).reshape(count_y, columns, modes)
        tx = jnp.asarray(table_x)
        tx_t = jnp.asarray(table_x.transpose(0, 2, 1) / np.float32(total_x * total_y))
        ty = jnp.asarray(table_y)
        ty_t = jnp.asarray(table_y.transpose(0, 2, 1))
        packed = pltpu.VMEM((modes, half * modes), jnp.float32)
        cube = pltpu.VMEM((levels, rows, columns), jnp.float32)
        dma = pltpu.SemaphoreType.DMA

        block, keep, send = call(
            forward_kernel,
            "forward",
            [(field, HBM), (tx_t, HBM), (ty, HBM)],
            (cube, packed, packed),
            [
                pltpu.VMEM(tx_t.shape[1:], jnp.float32),
                pltpu.VMEM(ty.shape[1:], jnp.float32),
                dma((6,)),
            ],
        )
        total = keep + swap(send, count_y)
        goal, mask, lift, tx, ty_t = call(
            prepare_kernel,
            "prepare",
            [
                (total, VMEM),
                (keep_count, SMEM),
                (level_class, SMEM),
                (height_table, SMEM),
                (drive, HBM),
                (tx, HBM),
                (ty_t, HBM),
            ],
            (
                packed,
                packed,
                pltpu.VMEM((levels, LANES), jnp.float32),
                pltpu.VMEM(tx.shape[1:], jnp.float32),
                pltpu.VMEM(ty_t.shape[1:], jnp.float32),
            ),
            [pltpu.VMEM((half, modes, modes), jnp.float32), dma((3,))],
            flops=10**9,
        )
        parts = [total]
        for stage in stages:
            if len(parts) > 1:
                parts = [sum(parts[1:], parts[0])]
            parts = parts + [swap(parts[0], bits) for bits in stage]
        delta, energy = call(
            settle_kernel,
            "settle",
            [(x, VMEM) for x in (goal, mask, *parts)],
            (packed, pltpu.VMEM((16, LANES), jnp.float32)),
        )
        energy = energy + swap(energy, count_y)
        increment = call(
            inverse_kernel,
            "inverse",
            [(x, VMEM) for x in (delta, swap(delta, count_y), lift, tx, ty_t)],
            cube,
            flops=3 * 10**9,
        )
        steps = count_v.bit_length() - 1
        for b in range(steps - 1):
            energy = energy + swap_var(energy, 1 << b)
        last = swap_var(energy, count_v // 2) if steps else jnp.zeros_like(energy)
        return call(
            finish_kernel,
            "finish",
            [(x, VMEM) for x in (energy, last, block, increment)],
            jax.ShapeDtypeStruct(field.shape, jnp.float32),
            [pltpu.VMEM((levels, rows, columns), jnp.float32), dma((4,))],
        )

    return jax.shard_map(
        per_device,
        mesh=mesh,
        in_specs=(P("var", None, "gx", "gy"), P("var", None, None, None), P(), P(), P()),
        out_specs=P("var", None, "gx", "gy"),
        check_vma=False,
    )
```

```python
import functools

import numpy as np

import jax
import jax.numpy as jnp
from jax import lax
from jax.experimental import pallas as pl
from jax.experimental.pallas import tpu as pltpu
from jax.sharding import PartitionSpec as P

energy_weights = (1.0, 1.0, 2.0, 3.0)
strength_top = 0.5
epsilon = 1e-06


LANES = 128
VMEM = pltpu.MemorySpace.VMEM
SMEM = pltpu.MemorySpace.SMEM
HBM = pltpu.MemorySpace.HBM


def cosine_table(total, modes):
    cells = np.arange(total, dtype=np.int64)
    waves = np.arange(modes, dtype=np.int64)
    phase = waves[None, :] * (2 * cells[:, None] + 1) % (4 * total)
    factor = np.where(waves == 0, 1.0, np.sqrt(2.0))
    return (np.cos(np.pi * phase / (2.0 * total)) * factor[None, :]).astype(np.float32)


def dot(a, b):
    return jnp.dot(a, b, preferred_element_type=jnp.float32)


def split(x):
    high = x.astype(jnp.bfloat16)
    return high, (x - high.astype(jnp.float32)).astype(jnp.bfloat16)


def stack_split(x, axis):
    return jnp.concatenate(split(x), axis=axis)


def split_table(table, axis):
    high = table.astype(jnp.bfloat16)
    low = (table - high.astype(np.float32)).astype(jnp.bfloat16)
    top = np.concatenate([high, high], axis=axis)
    return np.concatenate([top, np.concatenate([low, np.zeros_like(low)], axis=axis)], axis=3 - axis)


def pack_lanes(pieces, modes):
    tiles = -(-len(pieces) * modes // LANES)
    out = [None] * tiles
    lane = lax.broadcasted_iota(jnp.int32, pieces[0].shape, 1)

    def put(tile, value):
        out[tile] = value if out[tile] is None else out[tile] + value

    for index, piece in enumerate(pieces):
        tile, offset = divmod(index * modes, LANES)
        turned = pltpu.roll(piece, offset, 1) if offset else piece
        if offset + modes > LANES:
            put(tile, jnp.where(lane >= offset, turned, 0.0))
            put(tile + 1, jnp.where(lane < offset, turned, 0.0))
        else:
            put(tile, turned)
    return out


def unpack_lanes(tiles, count, modes):
    lane = lax.broadcasted_iota(jnp.int32, tiles[0].shape, 1)
    pieces = []
    for index in range(count):
        tile, offset = divmod(index * modes, LANES)
        piece = tiles[tile]
        if offset + modes > LANES:
            piece = jnp.where(lane >= offset, piece, tiles[tile + 1])
        pieces.append(pltpu.roll(piece, LANES - offset, 1) if offset else piece)
    return pieces


def transform(block, tx, ty, modes):
    wide = stack_split(jnp.concatenate(block, axis=1), 0)
    both = dot(tx, wide)
    part = both[:modes] + both[modes:]
    tall = jnp.concatenate([part[:, l * LANES : (l + 1) * LANES] for l in range(len(block))], axis=0)
    both = dot(stack_split(tall, 1), ty)
    coeff = both[:, :LANES] + both[:, LANES:]
    return [coeff[l * modes : (l + 1) * modes] for l in range(len(block))]


def store_packed(out_ref, pieces, modes):
    for t, tile in enumerate(pack_lanes(pieces, modes)):
        out_ref[:, t * LANES : (t + 1) * LANES] = tile


def send_kernel(field_ref, tx_ref, ty_ref, block_ref, send_ref, tx, ty, sems):
    half = block_ref.shape[0] // 2
    modes = send_ref.shape[0]
    at_x, at_y = lax.axis_index("gx"), lax.axis_index("gy")
    core = lax.rem(at_x, 2)
    first = (1 - core) * half
    starts = [(1 - core) * half, (1 - core) * half + half // 2, core * half]
    copies = [
        pltpu.make_async_copy(tx_ref.at[at_x], tx, sems.at[0]),
        pltpu.make_async_copy(ty_ref.at[at_y], ty, sems.at[1]),
    ]
    for q, (start, size) in enumerate(zip(starts, (half // 2, half // 2, half))):
        rows = pl.ds(start, size)
        copies.append(
            pltpu.make_async_copy(field_ref.at[0, rows], block_ref.at[rows], sems.at[2 + q])
        )
    for copy in copies:
        copy.start()
    copies[0].wait()
    copies[1].wait()
    pieces = []
    for q in range(2):
        copies[2 + q].wait()
        levels = [block_ref[first + l] for l in range(q * (half // 2), (q + 1) * (half // 2))]
        pieces += transform(levels, tx[...], ty[...], modes)
    store_packed(send_ref, pieces, modes)
    copies[4].wait()


def keep_kernel(block_ref, tx_ref, ty_ref, keep_ref):
    half = block_ref.shape[0] // 2
    modes = keep_ref.shape[0]
    first = lax.rem(lax.axis_index("gx"), 2) * half
    levels = [block_ref[first + l] for l in range(half)]
    store_packed(keep_ref, transform(levels, tx_ref[...], ty_ref[...], modes), modes)


def prepare_kernel(
    _,
    keep_count_ref,
    class_ref,
    height_ref,
    drive_ref,
    tx_ref,
    ty_ref,
    goal_ref,
    mask_ref,
    lift_ref,
    tx_out_ref,
    ty_out_ref,
    drive,
    sems,
):
    half, modes, _ = drive.shape
    width = goal_ref.shape[1]
    at_x, at_y = lax.axis_index("gx"), lax.axis_index("gy")
    first = lax.rem(at_x, 2) * half
    copies = [
        pltpu.make_async_copy(drive_ref.at[0, pl.ds(first, half)], drive, sems.at[0]),
        pltpu.make_async_copy(tx_ref.at[at_x], tx_out_ref, sems.at[1]),
        pltpu.make_async_copy(ty_ref.at[at_y], ty_out_ref, sems.at[2]),
    ]
    for copy in copies:
        copy.start()
    for l in range(lift_ref.shape[0]):
        lift_ref[l : l + 1, :] = jnp.full((1, LANES), height_ref[class_ref[l]], jnp.float32)
    lane = lax.broadcasted_iota(jnp.int32, (8, LANES), 1)
    row = lax.broadcasted_iota(jnp.int32, (8, LANES), 0)
    for t in range(width // LANES):
        limit = jnp.zeros((8, LANES), jnp.int32)
        for l in range(t * LANES // modes, min(half, ((t + 1) * LANES - 1) // modes + 1)):
            wave = lane + (t * LANES - l * modes)
            limit = jnp.where(wave >= 0, keep_count_ref[first + l] - wave, limit)
        for r in range(0, modes, 8):
            mask_ref[r : r + 8, t * LANES : (t + 1) * LANES] = (row + r < limit).astype(jnp.float32)
    copies[0].wait()
    pad = jnp.zeros((modes, LANES - modes), jnp.float32)
    goal = pack_lanes([jnp.concatenate([drive[l], pad], axis=1) for l in range(half)], modes)
    for t, tile in enumerate(goal):
        goal_ref[:, t * LANES : (t + 1) * LANES] = tile
    for copy in copies[1:]:
        copy.wait()


def settle_kernel(goal_ref, mask_ref, own_ref, *rest):
    *others, delta_ref, energy_ref = rest
    modes, width = own_ref.shape
    variable = lax.axis_index("var")
    weight = jnp.float32(0.0)
    for index, value in enumerate(energy_weights):
        weight = jnp.where(variable == index, jnp.float32(value), weight)
    gap = jnp.zeros((8, LANES), jnp.float32)
    model = jnp.zeros((8, LANES), jnp.float32)
    for t in range(width // LANES):
        for r in range(0, modes, 8):
            at = (slice(r, r + 8), slice(t * LANES, (t + 1) * LANES))
            coeff = own_ref[at]
            for other in others:
                coeff = coeff + other[at]
            mask = mask_ref[at]
            delta = mask * (goal_ref[at] - coeff)
            delta_ref[at] = delta
            gap = gap + delta * delta
            model = model + mask * coeff * coeff
    energy_ref[0:8, :] = weight * gap
    energy_ref[8:16, :] = weight * model


def inverse_kernel(which, delta_ref, lift_ref, tx_ref, ty_ref, out_ref):
    half, rows, _ = out_ref.shape
    modes, width = delta_ref.shape
    first = jnp.bitwise_xor(lax.rem(lax.axis_index("gx"), 2), which) * half
    tiles = [delta_ref[:, t * LANES : (t + 1) * LANES] for t in range(width // LANES)]
    tall = jnp.concatenate(unpack_lanes(tiles, half, modes), axis=0)
    both = dot(stack_split(tall, 1), ty_ref[...])
    back = both[:, :LANES] + both[:, LANES:]
    wide = jnp.concatenate([back[l * modes : (l + 1) * modes] for l in range(half)], axis=1)
    both = dot(tx_ref[...], stack_split(wide, 0))
    for l in range(half):
        at = slice(l * LANES, (l + 1) * LANES)
        out_ref[l] = lift_ref[pl.ds(first + l, 1), :] * (both[:rows, at] + both[rows:, at])


def finish_kernel(energy_ref, last_ref, block_ref, own_ref, other_ref, out_ref, buffer, sems):
    half = own_ref.shape[0]
    core = lax.rem(lax.axis_index("gx"), 2)
    energy = energy_ref[...] + last_ref[...]
    gap = jnp.sum(energy[:8], keepdims=True)
    model = jnp.sum(energy[8:], keepdims=True)
    strength = strength_top * gap / (gap + model + epsilon)
    count = sems.shape[0] // 2
    size = half // count
    copies = []
    for h, (ref, first) in enumerate(((own_ref, core * half), (other_ref, (1 - core) * half))):
        for q in range(count):
            for l in range(q * size, (q + 1) * size):
                buffer[h * half + l] = block_ref[first + l] + strength * ref[l]
            copies.append(
                pltpu.make_async_copy(
                    buffer.at[pl.ds(h * half + q * size, size)],
                    out_ref.at[0, pl.ds(first + q * size, size)],
                    sems.at[h * count + q],
                )
            )
            copies[-1].start()
    for copy in copies:
        copy.wait()


def call(kernel, name, ins, outs, scratch=(), flops=0):
    return pl.pallas_call(
        kernel,
        out_shape=outs,
        in_specs=[pl.BlockSpec(memory_space=pl.ANY if s is HBM else s) for _, s in ins],
        out_specs=jax.tree.map(
            lambda o: pl.BlockSpec(memory_space=VMEM if isinstance(o, pl.MemoryRef) else pl.ANY),
            outs,
            is_leaf=lambda o: isinstance(o, (pl.MemoryRef, jax.ShapeDtypeStruct)),
        ),
        scratch_shapes=scratch,
        cost_estimate=pl.CostEstimate(flops=flops, transcendentals=0, bytes_accessed=0),
        name=name,
    )(*[pltpu.with_memory_space_constraint(x, VMEM) if s is VMEM else x for x, s in ins])


def solution(mesh):
    count_x, count_y, count_v = (mesh.shape[a] for a in ("gx", "gy", "var"))
    ranks = count_x * count_y
    for count in (count_x, count_y, count_v):
        assert count & (count - 1) == 0

    def swap(value, bits):
        return lax.ppermute(value, ("gx", "gy"), [(i, i ^ bits) for i in range(ranks)])

    def swap_var(value, bits):
        return lax.ppermute(value, "var", [(i, i ^ bits) for i in range(count_v)])

    bits_x = [count_y << b for b in range(1, count_x.bit_length() - 1)]
    bits_y = [1 << b for b in range(count_y.bit_length() - 1)]
    stages = []
    for b in range(max(len(bits_x), len(bits_y))):
        bx, by = bits_x[b : b + 1], bits_y[b : b + 1]
        stages.append(bx + by + [x | y for x in bx for y in by])

    def per_device(field, drive, keep_count, level_class, height_table):
        _, levels, rows, columns = field.shape
        modes = drive.shape[-1]
        half = levels // 2
        total_x, total_y = rows * count_x, columns * count_y
        assert columns == LANES and levels % 4 == 0 and half * modes % LANES == 0 and modes % 8 == 0
        table_x = cosine_table(total_x, modes).reshape(count_x, rows, modes)
        table_y = np.zeros((count_y, columns, LANES), np.float32)
        table_y[:, :, :modes] = cosine_table(total_y, modes).reshape(count_y, columns, modes)
        tx_t = split_table(table_x.transpose(0, 2, 1) / np.float32(total_x * total_y), 2)
        ty = split_table(table_y, 1)
        tx = split_table(table_x, 2)
        ty_t = split_table(table_y.transpose(0, 2, 1), 1)
        packed = pltpu.VMEM((modes, half * modes), jnp.float32)
        cube = pltpu.VMEM((levels, rows, columns), jnp.float32)
        half_cube = pltpu.VMEM((half, rows, columns), jnp.float32)
        dma = pltpu.SemaphoreType.DMA
        like = lambda table: pltpu.VMEM(table.shape[1:], table.dtype)

        block, send, tx_t, ty = call(
            send_kernel,
            "send",
            [(field, HBM), (jnp.asarray(tx_t), HBM), (jnp.asarray(ty), HBM)],
            (cube, packed, like(tx_t), like(ty)),
            [dma((5,))],
        )
        keep = call(
            keep_kernel, "keep", [(x, VMEM) for x in (block, tx_t, ty)], packed, flops=10**9
        )
        total = keep + swap(send, count_y)
        goal, mask, lift, tx, ty_t = call(
            prepare_kernel,
            "prepare",
            [
                (total, VMEM),
                (keep_count, SMEM),
                (level_class, SMEM),
                (height_table, SMEM),
                (drive, HBM),
                (jnp.asarray(tx), HBM),
                (jnp.asarray(ty_t), HBM),
            ],
            (
                packed,
                packed,
                pltpu.VMEM((levels, LANES), jnp.float32),
                like(tx),
                like(ty_t),
            ),
            [pltpu.VMEM((half, modes, modes), jnp.float32), dma((3,))],
            flops=10**9,
        )
        parts = [total]
        for stage in stages:
            if len(parts) > 1:
                parts = [sum(parts[1:], parts[0])]
            parts = parts + [swap(parts[0], bits) for bits in stage]
        delta, energy = call(
            settle_kernel,
            "settle",
            [(x, VMEM) for x in (goal, mask, *parts)],
            (packed, pltpu.VMEM((16, LANES), jnp.float32)),
        )
        energy = energy + swap(energy, count_y)
        own, other = (
            call(
                functools.partial(inverse_kernel, which),
                name,
                [(x, VMEM) for x in (part, lift, tx, ty_t)],
                half_cube,
                flops=10**9,
            )
            for which, name, part in ((0, "inverse_own", delta), (1, "inverse_other", swap(delta, count_y)))
        )
        steps = count_v.bit_length() - 1
        for b in range(steps - 1):
            energy = energy + swap_var(energy, 1 << b)
        last = swap_var(energy, count_v // 2) if steps else jnp.zeros_like(energy)
        return call(
            finish_kernel,
            "finish",
            [(x, VMEM) for x in (energy, last, block, own, other)],
            jax.ShapeDtypeStruct(field.shape, jnp.float32),
            [pltpu.VMEM((levels, rows, columns), jnp.float32), dma((4,))],
        )

    return jax.shard_map(
        per_device,
        mesh=mesh,
        in_specs=(P("var", None, "gx", "gy"), P("var", None, None, None), P(), P(), P()),
        out_specs=P("var", None, "gx", "gy"),
        check_vma=False,
    )
```

```python
import functools

import numpy as np

import jax
import jax.numpy as jnp
from jax import lax
from jax.experimental import pallas as pl
from jax.experimental.pallas import tpu as pltpu
from jax.sharding import PartitionSpec as P

energy_weights = (1.0, 1.0, 2.0, 3.0)
strength_top = 0.5
epsilon = 1e-06


LANES = 128
VMEM = pltpu.MemorySpace.VMEM
SMEM = pltpu.MemorySpace.SMEM
HBM = pltpu.MemorySpace.HBM


def cosine_table(total, modes):
    cells = np.arange(total, dtype=np.int64)
    waves = np.arange(modes, dtype=np.int64)
    phase = waves[None, :] * (2 * cells[:, None] + 1) % (4 * total)
    factor = np.where(waves == 0, 1.0, np.sqrt(2.0))
    return (np.cos(np.pi * phase / (2.0 * total)) * factor[None, :]).astype(np.float32)


def dot(a, b):
    return jnp.dot(a, b, preferred_element_type=jnp.float32)


def split(x):
    high = x.astype(jnp.bfloat16)
    return high, (x - high.astype(jnp.float32)).astype(jnp.bfloat16)


def stack_split(x, axis):
    return jnp.concatenate(split(x), axis=axis)


def split_table(table, axis):
    high = table.astype(jnp.bfloat16)
    low = (table - high.astype(np.float32)).astype(jnp.bfloat16)
    top = np.concatenate([high, high], axis=axis)
    return np.concatenate([top, np.concatenate([low, np.zeros_like(low)], axis=axis)], axis=3 - axis)


def owned_half():
    at_x, at_y = lax.axis_index("gx"), lax.axis_index("gy")
    return lax.rem(at_x + at_x // 2 + at_y, 2)


def pack_lanes(pieces, modes):
    tiles = -(-len(pieces) * modes // LANES)
    out = [None] * tiles
    lane = lax.broadcasted_iota(jnp.int32, pieces[0].shape, 1)

    def put(tile, value):
        out[tile] = value if out[tile] is None else out[tile] + value

    for index, piece in enumerate(pieces):
        tile, offset = divmod(index * modes, LANES)
        turned = pltpu.roll(piece, offset, 1) if offset else piece
        if offset + modes > LANES:
            put(tile, jnp.where(lane >= offset, turned, 0.0))
            put(tile + 1, jnp.where(lane < offset, turned, 0.0))
        else:
            put(tile, turned)
    return out


def unpack_lanes(tiles, count, modes):
    lane = lax.broadcasted_iota(jnp.int32, tiles[0].shape, 1)
    pieces = []
    for index in range(count):
        tile, offset = divmod(index * modes, LANES)
        piece = tiles[tile]
        if offset + modes > LANES:
            piece = jnp.where(lane >= offset, piece, tiles[tile + 1])
        pieces.append(pltpu.roll(piece, LANES - offset, 1) if offset else piece)
    return pieces


def transform(block, tx, ty, modes):
    wide = stack_split(jnp.concatenate(block, axis=1), 0)
    both = dot(tx, wide)
    part = both[:modes] + both[modes:]
    tall = jnp.concatenate([part[:, l * LANES : (l + 1) * LANES] for l in range(len(block))], axis=0)
    both = dot(stack_split(tall, 1), ty)
    coeff = both[:, :LANES] + both[:, LANES:]
    return [coeff[l * modes : (l + 1) * modes] for l in range(len(block))]


def store_packed(out_ref, pieces, modes):
    for t, tile in enumerate(pack_lanes(pieces, modes)):
        out_ref[:, t * LANES : (t + 1) * LANES] = tile


def send_kernel(field_ref, tx_ref, ty_ref, block_ref, send_ref, tx, ty, sems):
    half = block_ref.shape[0] // 2
    modes = send_ref.shape[0]
    at_x, at_y = lax.axis_index("gx"), lax.axis_index("gy")
    core = owned_half()
    first = (1 - core) * half
    starts = [first, core * half]
    copies = [
        pltpu.make_async_copy(tx_ref.at[at_x], tx, sems.at[0]),
        pltpu.make_async_copy(ty_ref.at[at_y], ty, sems.at[1]),
    ]
    for q, (start, size) in enumerate(zip(starts, (half, half))):
        rows = pl.ds(start, size)
        copies.append(
            pltpu.make_async_copy(field_ref.at[0, rows], block_ref.at[rows], sems.at[2 + q])
        )
    for copy in copies:
        copy.start()
    copies[0].wait()
    copies[1].wait()
    pieces = []
    for q in range(1):
        copies[2 + q].wait()
        levels = [block_ref[first + l] for l in range(half)]
        pieces += transform(levels, tx[...], ty[...], modes)
    store_packed(send_ref, pieces, modes)
    copies[3].wait()


def keep_kernel(block_ref, tx_ref, ty_ref, keep_ref):
    half = block_ref.shape[0] // 2
    modes = keep_ref.shape[0]
    first = owned_half() * half
    levels = [block_ref[first + l] for l in range(half)]
    store_packed(keep_ref, transform(levels, tx_ref[...], ty_ref[...], modes), modes)


def prepare_kernel(
    _,
    keep_count_ref,
    class_ref,
    height_ref,
    drive_ref,
    tx_ref,
    ty_ref,
    goal_ref,
    mask_ref,
    lift_ref,
    tx_out_ref,
    ty_out_ref,
    drive,
    sems,
):
    half, modes, _ = drive.shape
    width = goal_ref.shape[1]
    at_x, at_y = lax.axis_index("gx"), lax.axis_index("gy")
    first = owned_half() * half
    copies = [
        pltpu.make_async_copy(drive_ref.at[0, pl.ds(first, half)], drive, sems.at[0]),
        pltpu.make_async_copy(tx_ref.at[at_x], tx_out_ref, sems.at[1]),
        pltpu.make_async_copy(ty_ref.at[at_y], ty_out_ref, sems.at[2]),
    ]
    for copy in copies:
        copy.start()
    for l in range(lift_ref.shape[0]):
        lift_ref[l : l + 1, :] = jnp.full((1, LANES), height_ref[class_ref[l]], jnp.float32)
    lane = lax.broadcasted_iota(jnp.int32, (8, LANES), 1)
    row = lax.broadcasted_iota(jnp.int32, (8, LANES), 0)
    for t in range(width // LANES):
        limit = jnp.zeros((8, LANES), jnp.int32)
        for l in range(t * LANES // modes, min(half, ((t + 1) * LANES - 1) // modes + 1)):
            wave = lane + (t * LANES - l * modes)
            limit = jnp.where(wave >= 0, keep_count_ref[first + l] - wave, limit)
        for r in range(0, modes, 8):
            mask_ref[r : r + 8, t * LANES : (t + 1) * LANES] = (row + r < limit).astype(jnp.float32)
    copies[0].wait()
    pad = jnp.zeros((modes, LANES - modes), jnp.float32)
    goal = pack_lanes([jnp.concatenate([drive[l], pad], axis=1) for l in range(half)], modes)
    for t, tile in enumerate(goal):
        goal_ref[:, t * LANES : (t + 1) * LANES] = tile
    for copy in copies[1:]:
        copy.wait()


def settle_kernel(goal_ref, mask_ref, own_ref, *rest):
    *others, delta_ref, energy_ref = rest
    modes, width = own_ref.shape
    variable = lax.axis_index("var")
    weight = jnp.float32(0.0)
    for index, value in enumerate(energy_weights):
        weight = jnp.where(variable == index, jnp.float32(value), weight)
    gap = jnp.zeros((8, LANES), jnp.float32)
    model = jnp.zeros((8, LANES), jnp.float32)
    for t in range(width // LANES):
        for r in range(0, modes, 8):
            at = (slice(r, r + 8), slice(t * LANES, (t + 1) * LANES))
            coeff = own_ref[at]
            for other in others:
                coeff = coeff + other[at]
            mask = mask_ref[at]
            delta = mask * (goal_ref[at] - coeff)
            delta_ref[at] = delta
            gap = gap + delta * delta
            model = model + mask * coeff * coeff
    gap = jnp.sum(gap, axis=0, keepdims=True)
    model = jnp.sum(model, axis=0, keepdims=True)
    energy_ref[...] = weight * jnp.where(lax.broadcasted_iota(jnp.int32, (8, LANES), 0) == 0, gap, model)


def inverse_kernel(which, delta_ref, lift_ref, tx_ref, ty_ref, out_ref):
    half, rows, _ = out_ref.shape
    modes, width = delta_ref.shape
    first = jnp.bitwise_xor(owned_half(), which) * half
    tiles = [delta_ref[:, t * LANES : (t + 1) * LANES] for t in range(width // LANES)]
    tall = jnp.concatenate(unpack_lanes(tiles, half, modes), axis=0)
    both = dot(stack_split(tall, 1), ty_ref[...])
    back = both[:, :LANES] + both[:, LANES:]
    wide = jnp.concatenate([back[l * modes : (l + 1) * modes] for l in range(half)], axis=1)
    both = dot(tx_ref[...], stack_split(wide, 0))
    for l in range(half):
        at = slice(l * LANES, (l + 1) * LANES)
        out_ref[l] = lift_ref[pl.ds(first + l, 1), :] * (both[:rows, at] + both[rows:, at])


def finish_kernel(energy_ref, last_ref, block_ref, own_ref, other_ref, out_ref, buffer, sems):
    half = own_ref.shape[0]
    core = owned_half()
    energy = energy_ref[...] + last_ref[...]
    gap = jnp.sum(energy[:1], keepdims=True)
    model = jnp.sum(energy[1:2], keepdims=True)
    strength = strength_top * gap / (gap + model + epsilon)
    count = sems.shape[0] // 2
    size = half // count
    copies = []
    for h, (ref, first) in enumerate(((own_ref, core * half), (other_ref, (1 - core) * half))):
        for q in range(count):
            for l in range(q * size, (q + 1) * size):
                buffer[h * half + l] = block_ref[first + l] + strength * ref[l]
            copies.append(
                pltpu.make_async_copy(
                    buffer.at[pl.ds(h * half + q * size, size)],
                    out_ref.at[0, pl.ds(first + q * size, size)],
                    sems.at[h * count + q],
                )
            )
            copies[-1].start()
    for copy in copies:
        copy.wait()


def call(kernel, name, ins, outs, scratch=(), flops=0):
    return pl.pallas_call(
        kernel,
        out_shape=outs,
        in_specs=[pl.BlockSpec(memory_space=pl.ANY if s is HBM else s) for _, s in ins],
        out_specs=jax.tree.map(
            lambda o: pl.BlockSpec(memory_space=VMEM if isinstance(o, pl.MemoryRef) else pl.ANY),
            outs,
            is_leaf=lambda o: isinstance(o, (pl.MemoryRef, jax.ShapeDtypeStruct)),
        ),
        scratch_shapes=scratch,
        cost_estimate=pl.CostEstimate(flops=flops, transcendentals=0, bytes_accessed=0),
        name=name,
    )(*[pltpu.with_memory_space_constraint(x, VMEM) if s is VMEM else x for x, s in ins])


def solution(mesh):
    count_x, count_y, count_v = (mesh.shape[a] for a in ("gx", "gy", "var"))
    ranks = count_x * count_y
    for count in (count_x, count_y, count_v):
        assert count & (count - 1) == 0

    def swap(value, bits, bits_v=0):
        bits = bits * count_v + bits_v
        pairs = [(i, i ^ bits) for i in range(ranks * count_v)]
        return lax.ppermute(value, ("gx", "gy", "var"), pairs)

    core = count_y

    bits_x = [count_y << b for b in range(1, count_x.bit_length() - 1)]
    bits_y = [1 << b for b in range(count_y.bit_length() - 1)]
    stages = []
    for b in range(max(len(bits_x), len(bits_y))):
        bx, by = bits_x[b : b + 1], bits_y[b : b + 1]
        stages.append([bits | core * ((bits + bits // (2 * core)) % 2) for bits in bx + by + [x | y for x in bx for y in by]])

    def per_device(field, drive, keep_count, level_class, height_table):
        _, levels, rows, columns = field.shape
        modes = drive.shape[-1]
        half = levels // 2
        total_x, total_y = rows * count_x, columns * count_y
        assert columns == LANES and levels % 4 == 0 and half * modes % LANES == 0 and modes % 8 == 0
        table_x = cosine_table(total_x, modes).reshape(count_x, rows, modes)
        table_y = np.zeros((count_y, columns, LANES), np.float32)
        table_y[:, :, :modes] = cosine_table(total_y, modes).reshape(count_y, columns, modes)
        tx_t = split_table(table_x.transpose(0, 2, 1) / np.float32(total_x * total_y), 2)
        ty = split_table(table_y, 1)
        tx = split_table(table_x, 2)
        ty_t = split_table(table_y.transpose(0, 2, 1), 1)
        packed = pltpu.VMEM((modes, half * modes), jnp.float32)
        cube = pltpu.VMEM((levels, rows, columns), jnp.float32)
        half_cube = pltpu.VMEM((half, rows, columns), jnp.float32)
        dma = pltpu.SemaphoreType.DMA
        like = lambda table: pltpu.VMEM(table.shape[1:], table.dtype)

        block, send, tx_t, ty = call(
            send_kernel,
            "send",
            [(field, HBM), (jnp.asarray(tx_t), HBM), (jnp.asarray(ty), HBM)],
            (cube, packed, like(tx_t), like(ty)),
            [dma((5,))],
        )
        keep = call(
            keep_kernel, "keep", [(x, VMEM) for x in (block, tx_t, ty)], packed, flops=10**9
        )
        total = keep + swap(send, core)
        goal, mask, lift, tx, ty_t = call(
            prepare_kernel,
            "prepare",
            [
                (total, VMEM),
                (keep_count, SMEM),
                (level_class, SMEM),
                (height_table, SMEM),
                (drive, HBM),
                (jnp.asarray(tx), HBM),
                (jnp.asarray(ty_t), HBM),
            ],
            (
                packed,
                packed,
                pltpu.VMEM((levels, LANES), jnp.float32),
                like(tx),
                like(ty_t),
            ),
            [pltpu.VMEM((half, modes, modes), jnp.float32), dma((3,))],
            flops=10**9,
        )
        parts = [total]
        for stage in stages:
            if len(parts) > 1:
                parts = [sum(parts[1:], parts[0])]
            parts = parts + [swap(parts[0], bits) for bits in stage]
        delta, energy = call(
            settle_kernel,
            "settle",
            [(x, VMEM) for x in (goal, mask, *parts)],
            (packed, pltpu.VMEM((8, LANES), jnp.float32)),
        )
        energy = energy + swap(energy, core)
        late, energy = lax.optimization_barrier((delta, energy))
        own, other = (
            call(
                functools.partial(inverse_kernel, which),
                name,
                [(x, VMEM) for x in (part, lift, tx, ty_t)],
                half_cube,
                flops=10**9,
            )
            for which, name, part in ((0, "inverse_own", delta), (1, "inverse_other", swap(late, core)))
        )
        steps = count_v.bit_length() - 1
        for b in range(steps - 1):
            energy = energy + swap(energy, core, 1 << b)
        last = swap(energy, core, count_v // 2) if steps else jnp.zeros_like(energy)
        return call(
            finish_kernel,
            "finish",
            [(x, VMEM) for x in (energy, last, block, own, other)],
            jax.ShapeDtypeStruct(field.shape, jnp.float32),
            [pltpu.VMEM((levels, rows, columns), jnp.float32), dma((4,))],
        )

    return jax.shard_map(
        per_device,
        mesh=mesh,
        in_specs=(P("var", None, "gx", "gy"), P("var", None, None, None), P(), P(), P()),
        out_specs=P("var", None, "gx", "gy"),
        check_vma=False,
    )
```

```python
import functools

import numpy as np

import jax
import jax.numpy as jnp
from jax import lax
from jax.experimental import pallas as pl
from jax.experimental.pallas import tpu as pltpu
from jax.sharding import PartitionSpec as P


energy_weights = (1.0, 1.0, 2.0, 3.0)
strength_top = 0.5
epsilon = 1e-06


LANES = 128
VMEM = pltpu.MemorySpace.VMEM
SMEM = pltpu.MemorySpace.SMEM
HBM = pltpu.MemorySpace.HBM


def cosine_table(total, modes):
    cells = np.arange(total, dtype=np.int64)
    waves = np.arange(modes, dtype=np.int64)
    phase = waves[None, :] * (2 * cells[:, None] + 1) % (4 * total)
    factor = np.where(waves == 0, 1.0, np.sqrt(2.0))
    return (np.cos(np.pi * phase / (2.0 * total)) * factor[None, :]).astype(np.float32)


def dot(a, b):
    return jnp.dot(a, b, preferred_element_type=jnp.float32)


def split(x):
    high = x.astype(jnp.bfloat16)
    return high, (x - high.astype(jnp.float32)).astype(jnp.bfloat16)


def stack_split(x, axis):
    return jnp.concatenate(split(x), axis=axis)


def split_table(table, axis):
    high = table.astype(jnp.bfloat16)
    low = (table - high.astype(np.float32)).astype(jnp.bfloat16)
    top = np.concatenate([high, high], axis=axis)
    return np.concatenate([top, np.concatenate([low, np.zeros_like(low)], axis=axis)], axis=3 - axis)


def owned_half():
    at_x, at_y = lax.axis_index("gx"), lax.axis_index("gy")
    return lax.rem(at_x + at_x // 2 + at_y, 2)


def pack_lanes(pieces, modes):
    tiles = -(-len(pieces) * modes // LANES)
    out = [None] * tiles
    lane = lax.broadcasted_iota(jnp.int32, pieces[0].shape, 1)

    def put(tile, value):
        out[tile] = value if out[tile] is None else out[tile] + value

    for index, piece in enumerate(pieces):
        tile, offset = divmod(index * modes, LANES)
        turned = pltpu.roll(piece, offset, 1) if offset else piece
        if offset + modes > LANES:
            put(tile, jnp.where(lane >= offset, turned, 0.0))
            put(tile + 1, jnp.where(lane < offset, turned, 0.0))
        else:
            put(tile, turned)
    return out


def unpack_lanes(tiles, count, modes):
    lane = lax.broadcasted_iota(jnp.int32, tiles[0].shape, 1)
    pieces = []
    for index in range(count):
        tile, offset = divmod(index * modes, LANES)
        piece = tiles[tile]
        if offset + modes > LANES:
            piece = jnp.where(lane >= offset, piece, tiles[tile + 1])
        pieces.append(pltpu.roll(piece, LANES - offset, 1) if offset else piece)
    return pieces


def transform(block, tx, ty, modes):
    wide = stack_split(jnp.concatenate(block, axis=1), 0)
    both = dot(tx, wide)
    part = both[:modes] + both[modes:]
    tall = jnp.concatenate([part[:, l * LANES : (l + 1) * LANES] for l in range(len(block))], axis=0)
    both = dot(stack_split(tall, 1), ty)
    coeff = both[:, :LANES] + both[:, LANES:]
    return [coeff[l * modes : (l + 1) * modes] for l in range(len(block))]


def store_packed(out_ref, pieces, modes):
    for t, tile in enumerate(pack_lanes(pieces, modes)):
        out_ref[:, t * LANES : (t + 1) * LANES] = tile


def send_kernel(field_ref, tx_ref, ty_ref, block_ref, send_ref, tx, ty, sems):
    half = block_ref.shape[0] // 2
    modes = send_ref.shape[0]
    at_x, at_y = lax.axis_index("gx"), lax.axis_index("gy")
    core = owned_half()
    first = (1 - core) * half
    starts = [first, core * half]
    copies = [
        pltpu.make_async_copy(tx_ref.at[at_x], tx, sems.at[0]),
        pltpu.make_async_copy(ty_ref.at[at_y], ty, sems.at[1]),
    ]
    for q, (start, size) in enumerate(zip(starts, (half, half))):
        rows = pl.ds(start, size)
        copies.append(
            pltpu.make_async_copy(field_ref.at[0, rows], block_ref.at[rows], sems.at[2 + q])
        )
    for copy in copies:
        copy.start()
    copies[0].wait()
    copies[1].wait()
    pieces = []
    for q in range(1):
        copies[2 + q].wait()
        levels = [block_ref[first + l] for l in range(half)]
        pieces += transform(levels, tx[...], ty[...], modes)
    store_packed(send_ref, pieces, modes)
    copies[3].wait()


def keep_kernel(block_ref, tx_ref, ty_ref, keep_ref):
    half = block_ref.shape[0] // 2
    modes = keep_ref.shape[0]
    first = owned_half() * half
    levels = [block_ref[first + l] for l in range(half)]
    store_packed(keep_ref, transform(levels, tx_ref[...], ty_ref[...], modes), modes)


def prepare_kernel(
    _,
    keep_count_ref,
    class_ref,
    height_ref,
    drive_ref,
    tx_ref,
    ty_ref,
    goal_ref,
    mask_ref,
    lift_ref,
    tx_out_ref,
    ty_out_ref,
    drive,
    sems,
):
    half, modes, _ = drive.shape
    width = goal_ref.shape[1]
    at_x, at_y = lax.axis_index("gx"), lax.axis_index("gy")
    first = owned_half() * half
    copies = [
        pltpu.make_async_copy(drive_ref.at[0, pl.ds(first, half)], drive, sems.at[0]),
        pltpu.make_async_copy(tx_ref.at[at_x], tx_out_ref, sems.at[1]),
        pltpu.make_async_copy(ty_ref.at[at_y], ty_out_ref, sems.at[2]),
    ]
    for copy in copies:
        copy.start()
    for l in range(lift_ref.shape[0]):
        lift_ref[l : l + 1, :] = jnp.full((1, LANES), height_ref[class_ref[l]], jnp.float32)
    lane = lax.broadcasted_iota(jnp.int32, (8, LANES), 1)
    row = lax.broadcasted_iota(jnp.int32, (8, LANES), 0)
    for t in range(width // LANES):
        limit = jnp.zeros((8, LANES), jnp.int32)
        for l in range(t * LANES // modes, min(half, ((t + 1) * LANES - 1) // modes + 1)):
            wave = lane + (t * LANES - l * modes)
            limit = jnp.where(wave >= 0, keep_count_ref[first + l] - wave, limit)
        for r in range(0, modes, 8):
            mask_ref[r : r + 8, t * LANES : (t + 1) * LANES] = (row + r < limit).astype(jnp.float32)
    copies[0].wait()
    pad = jnp.zeros((modes, LANES - modes), jnp.float32)
    goal = pack_lanes([jnp.concatenate([drive[l], pad], axis=1) for l in range(half)], modes)
    for t, tile in enumerate(goal):
        goal_ref[:, t * LANES : (t + 1) * LANES] = tile
    for copy in copies[1:]:
        copy.wait()


def settle_kernel(goal_ref, mask_ref, own_ref, *rest):
    *others, delta_ref, energy_ref = rest
    modes, width = own_ref.shape
    variable = lax.axis_index("var")
    weight = jnp.float32(0.0)
    for index, value in enumerate(energy_weights):
        weight = jnp.where(variable == index, jnp.float32(value), weight)
    gap = jnp.zeros((8, LANES), jnp.float32)
    model = jnp.zeros((8, LANES), jnp.float32)
    for t in range(width // LANES):
        for r in range(0, modes, 8):
            at = (slice(r, r + 8), slice(t * LANES, (t + 1) * LANES))
            coeff = own_ref[at]
            for other in others:
                coeff = coeff + other[at]
            mask = mask_ref[at]
            delta = mask * (goal_ref[at] - coeff)
            delta_ref[at] = delta
            gap = gap + delta * delta
            model = model + mask * coeff * coeff
    gap = jnp.sum(gap, axis=0, keepdims=True)
    model = jnp.sum(model, axis=0, keepdims=True)
    energy_ref[...] = weight * jnp.where(lax.broadcasted_iota(jnp.int32, (8, LANES), 0) == 0, gap, model)


def inverse_kernel(which, delta_ref, lift_ref, tx_ref, ty_ref, out_ref):
    half, rows, _ = out_ref.shape
    modes, width = delta_ref.shape
    first = jnp.bitwise_xor(owned_half(), which) * half
    tiles = [delta_ref[:, t * LANES : (t + 1) * LANES] for t in range(width // LANES)]
    tall = jnp.concatenate(unpack_lanes(tiles, half, modes), axis=0)
    both = dot(stack_split(tall, 1), ty_ref[...])
    back = both[:, :LANES] + both[:, LANES:]
    wide = jnp.concatenate([back[l * modes : (l + 1) * modes] for l in range(half)], axis=1)
    both = dot(tx_ref[...], stack_split(wide, 0))
    for l in range(half):
        at = slice(l * LANES, (l + 1) * LANES)
        out_ref[l] = lift_ref[pl.ds(first + l, 1), :] * (both[:rows, at] + both[rows:, at])


def finish_kernel(energy_ref, last_ref, block_ref, own_ref, other_ref, out_ref, buffer, sems):
    half = own_ref.shape[0]
    core = owned_half()
    energy = energy_ref[...] + last_ref[...]
    gap = jnp.sum(energy[:1], keepdims=True)
    model = jnp.sum(energy[1:2], keepdims=True)
    strength = strength_top * gap / (gap + model + epsilon)
    count = sems.shape[0] // 2
    size = half // count
    copies = []
    for h, (ref, first) in enumerate(((own_ref, core * half), (other_ref, (1 - core) * half))):
        for q in range(count):
            for l in range(q * size, (q + 1) * size):
                buffer[h * half + l] = block_ref[first + l] + strength * ref[l]
            copies.append(
                pltpu.make_async_copy(
                    buffer.at[pl.ds(h * half + q * size, size)],
                    out_ref.at[0, pl.ds(first + q * size, size)],
                    sems.at[h * count + q],
                )
            )
            copies[-1].start()
    for copy in copies:
        copy.wait()


def call(kernel, ins, outs, scratch=(), flops=0):
    return pl.pallas_call(
        kernel,
        out_shape=outs,
        in_specs=[pl.BlockSpec(memory_space=pl.ANY if s is HBM else s) for _, s in ins],
        out_specs=jax.tree.map(
            lambda o: pl.BlockSpec(memory_space=VMEM if isinstance(o, pl.MemoryRef) else pl.ANY),
            outs,
            is_leaf=lambda o: isinstance(o, (pl.MemoryRef, jax.ShapeDtypeStruct)),
        ),
        scratch_shapes=scratch,
        cost_estimate=pl.CostEstimate(flops=flops, transcendentals=0, bytes_accessed=0),
    )(*[pltpu.with_memory_space_constraint(x, VMEM) if s is VMEM else x for x, s in ins])


def solution(mesh):
    count_x, count_y, count_v = (mesh.shape[a] for a in ("gx", "gy", "var"))
    ranks = count_x * count_y
    for count in (count_x, count_y, count_v):
        assert count & (count - 1) == 0

    def swap(value, bits, bits_v=0):
        bits = bits * count_v + bits_v
        pairs = [(i, i ^ bits) for i in range(ranks * count_v)]
        return lax.ppermute(value, ("gx", "gy", "var"), pairs)

    core = count_y

    bits_x = [count_y << b for b in range(1, count_x.bit_length() - 1)]
    bits_y = [1 << b for b in range(count_y.bit_length() - 1)]
    stages = []
    for b in range(max(len(bits_x), len(bits_y))):
        bx, by = bits_x[b : b + 1], bits_y[b : b + 1]
        stages.append([bits | core * ((bits + bits // (2 * core)) % 2) for bits in bx + by + [x | y for x in bx for y in by]])

    def nudge(field, drive, keep_count, level_class, height_table):
        _, levels, rows, columns = field.shape
        modes = drive.shape[-1]
        half = levels // 2
        total_x, total_y = rows * count_x, columns * count_y
        assert columns == LANES and levels % 4 == 0 and half * modes % LANES == 0 and modes % 8 == 0
        table_x = cosine_table(total_x, modes).reshape(count_x, rows, modes)
        table_y = np.zeros((count_y, columns, LANES), np.float32)
        table_y[:, :, :modes] = cosine_table(total_y, modes).reshape(count_y, columns, modes)
        tx_t = split_table(table_x.transpose(0, 2, 1) / np.float32(total_x * total_y), 2)
        ty = split_table(table_y, 1)
        tx = split_table(table_x, 2)
        ty_t = split_table(table_y.transpose(0, 2, 1), 1)
        packed = pltpu.VMEM((modes, half * modes), jnp.float32)
        cube = pltpu.VMEM((levels, rows, columns), jnp.float32)
        half_cube = pltpu.VMEM((half, rows, columns), jnp.float32)
        dma = pltpu.SemaphoreType.DMA
        like = lambda table: pltpu.VMEM(table.shape[1:], table.dtype)

        block, send, tx_t, ty = call(
            send_kernel,
            [(field, HBM), (jnp.asarray(tx_t), HBM), (jnp.asarray(ty), HBM)],
            (cube, packed, like(tx_t), like(ty)),
            [dma((5,))],
        )
        keep = call(keep_kernel, [(x, VMEM) for x in (block, tx_t, ty)], packed, flops=10**9)
        total = keep + swap(send, core)
        goal, mask, lift, tx, ty_t = call(
            prepare_kernel,
            [
                (total, VMEM),
                (keep_count, SMEM),
                (level_class, SMEM),
                (height_table, SMEM),
                (drive, HBM),
                (jnp.asarray(tx), HBM),
                (jnp.asarray(ty_t), HBM),
            ],
            (
                packed,
                packed,
                pltpu.VMEM((levels, LANES), jnp.float32),
                like(tx),
                like(ty_t),
            ),
            [pltpu.VMEM((half, modes, modes), jnp.float32), dma((3,))],
            flops=10**9,
        )
        parts = [total]
        for stage in stages:
            if len(parts) > 1:
                parts = [sum(parts[1:], parts[0])]
            parts = parts + [swap(parts[0], bits) for bits in stage]
        delta, energy = call(
            settle_kernel, [(x, VMEM) for x in (goal, mask, *parts)], (packed, pltpu.VMEM((8, LANES), jnp.float32))
        )
        energy = energy + swap(energy, core)
        shared = swap(delta, core)
        own, other = (
            call(
                functools.partial(inverse_kernel, which),
                [(x, VMEM) for x in (part, lift, tx, ty_t)],
                half_cube,
                flops=10**9,
            )
            for which, part in ((0, delta), (1, shared))
        )
        last = jnp.zeros_like(energy)
        for b in range(count_v.bit_length() - 1):
            energy = energy + last
            last = swap(energy, core, 1 << b)
        return call(
            finish_kernel,
            [(x, VMEM) for x in (energy, last, block, own, other)],
            jax.ShapeDtypeStruct(field.shape, jnp.float32),
            [pltpu.VMEM((levels, rows, columns), jnp.float32), dma((4,))],
        )

    return jax.shard_map(
        nudge,
        mesh=mesh,
        in_specs=(P("var", None, "gx", "gy"), P("var", None, None, None), P(), P(), P()),
        out_specs=P("var", None, "gx", "gy"),
        check_vma=False,
    )
```

```python
import functools

import numpy as np

import jax
import jax.numpy as jnp
from jax import lax
from jax.experimental import pallas as pl
from jax.experimental.pallas import tpu as pltpu
from jax.sharding import PartitionSpec as P


energy_weights = (1.0, 1.0, 2.0, 3.0)
strength_top = 0.5
epsilon = 1e-06


LANES = 128
VMEM = pltpu.MemorySpace.VMEM
SMEM = pltpu.MemorySpace.SMEM
HBM = pltpu.MemorySpace.HBM


def cosine_table(total, modes):
    cells = np.arange(total, dtype=np.int64)
    waves = np.arange(modes, dtype=np.int64)
    phase = waves[None, :] * (2 * cells[:, None] + 1) % (4 * total)
    factor = np.where(waves == 0, 1.0, np.sqrt(2.0))
    return (np.cos(np.pi * phase / (2.0 * total)) * factor[None, :]).astype(np.float32)


def dot(a, b):
    return jnp.dot(a, b, preferred_element_type=jnp.float32)


def split(x):
    high = x.astype(jnp.bfloat16)
    return high, (x - high.astype(jnp.float32)).astype(jnp.bfloat16)


def stack_split(x, axis):
    return jnp.concatenate(split(x), axis=axis)


def split_table(table, axis):
    high = table.astype(jnp.bfloat16)
    low = (table - high.astype(np.float32)).astype(jnp.bfloat16)
    both = np.concatenate([high, low], axis=3 - axis)
    return np.concatenate([both, both], axis=axis)


def owned_half():
    at_x, at_y = lax.axis_index("gx"), lax.axis_index("gy")
    return lax.rem(at_x + at_x // 2 + at_y, 2)


def pack_lanes(pieces, modes):
    tiles = -(-len(pieces) * modes // LANES)
    out = [None] * tiles
    lane = lax.broadcasted_iota(jnp.int32, pieces[0].shape, 1)

    def put(tile, value):
        out[tile] = value if out[tile] is None else out[tile] + value

    for index, piece in enumerate(pieces):
        tile, offset = divmod(index * modes, LANES)
        turned = pltpu.roll(piece, offset, 1) if offset else piece
        if offset + modes > LANES:
            put(tile, jnp.where(lane >= offset, turned, 0.0))
            put(tile + 1, jnp.where(lane < offset, turned, 0.0))
        else:
            put(tile, turned)
    return out


def unpack_lanes(tiles, count, modes):
    lane = lax.broadcasted_iota(jnp.int32, tiles[0].shape, 1)
    pieces = []
    for index in range(count):
        tile, offset = divmod(index * modes, LANES)
        piece = tiles[tile]
        if offset + modes > LANES:
            piece = jnp.where(lane >= offset, piece, tiles[tile + 1])
        pieces.append(pltpu.roll(piece, LANES - offset, 1) if offset else piece)
    return pieces


def transform(block, tx, ty_ref, modes, ready=lambda: None):
    wide = stack_split(jnp.concatenate(block, axis=1), 0)
    both = dot(tx, wide)
    part = both[:modes] + both[modes:]
    tall = jnp.concatenate([part[:, l * LANES : (l + 1) * LANES] for l in range(len(block))], axis=0)
    ready()
    both = dot(stack_split(tall, 1), ty_ref[...])
    coeff = both[:, :LANES] + both[:, LANES:]
    return [coeff[l * modes : (l + 1) * modes] for l in range(len(block))]


def store_packed(out_ref, pieces, modes):
    for t, tile in enumerate(pack_lanes(pieces, modes)):
        out_ref[:, t * LANES : (t + 1) * LANES] = tile


def send_kernel(field_ref, tx_ref, ty_ref, block_ref, send_ref, tx, ty, sems):
    half = block_ref.shape[0] // 2
    modes = send_ref.shape[0]
    owned = owned_half()
    first = (1 - owned) * half

    def levels_copy(start, sem):
        rows = pl.ds(start, half)
        return pltpu.make_async_copy(field_ref.at[0, rows], block_ref.at[rows], sem)

    sent = levels_copy(first, sems.at[0])
    kept = levels_copy(owned * half, sems.at[1])
    tx_copy = pltpu.make_async_copy(tx_ref.at[lax.axis_index("gx")], tx, sems.at[2])
    ty_copy = pltpu.make_async_copy(ty_ref.at[lax.axis_index("gy")], ty, sems.at[3])
    for copy in (sent, tx_copy, ty_copy, kept):
        copy.start()
    tx_copy.wait()
    sent.wait()
    levels = [block_ref[first + l] for l in range(half)]
    store_packed(send_ref, transform(levels, tx[...], ty, modes, ty_copy.wait), modes)
    kept.wait()


def keep_kernel(block_ref, tx_ref, ty_ref, keep_ref):
    half = block_ref.shape[0] // 2
    modes = keep_ref.shape[0]
    first = owned_half() * half
    levels = [block_ref[first + l] for l in range(half)]
    store_packed(keep_ref, transform(levels, tx_ref[...], ty_ref, modes), modes)


def prepare_kernel(
    _,
    keep_count_ref,
    class_ref,
    height_ref,
    drive_ref,
    tx_ref,
    ty_ref,
    goal_ref,
    mask_ref,
    lift_ref,
    tx_out_ref,
    ty_out_ref,
    drive,
    sems,
):
    half, modes, _ = drive.shape
    width = goal_ref.shape[1]
    at_x, at_y = lax.axis_index("gx"), lax.axis_index("gy")
    first = owned_half() * half
    copies = [
        pltpu.make_async_copy(drive_ref.at[0, pl.ds(first, half)], drive, sems.at[0]),
        pltpu.make_async_copy(tx_ref.at[at_x], tx_out_ref, sems.at[1]),
        pltpu.make_async_copy(ty_ref.at[at_y], ty_out_ref, sems.at[2]),
    ]
    for copy in copies:
        copy.start()
    for l in range(lift_ref.shape[0]):
        lift_ref[l : l + 1, :] = jnp.full((1, LANES), height_ref[class_ref[l]], jnp.float32)
    lane = lax.broadcasted_iota(jnp.int32, (8, LANES), 1)
    row = lax.broadcasted_iota(jnp.int32, (8, LANES), 0)
    for t in range(width // LANES):
        limit = jnp.zeros((8, LANES), jnp.int32)
        for l in range(t * LANES // modes, min(half, ((t + 1) * LANES - 1) // modes + 1)):
            wave = lane + (t * LANES - l * modes)
            limit = jnp.where(wave >= 0, keep_count_ref[first + l] - wave, limit)
        for r in range(0, modes, 8):
            mask_ref[r : r + 8, t * LANES : (t + 1) * LANES] = (row + r < limit).astype(jnp.float32)
    copies[0].wait()
    pad = jnp.zeros((modes, LANES - modes), jnp.float32)
    goal = pack_lanes([jnp.concatenate([drive[l], pad], axis=1) for l in range(half)], modes)
    for t, tile in enumerate(goal):
        goal_ref[:, t * LANES : (t + 1) * LANES] = tile
    for copy in copies[1:]:
        copy.wait()


def settle_kernel(goal_ref, mask_ref, own_ref, *rest):
    *others, delta_ref, energy_ref = rest
    modes, width = own_ref.shape
    variable = lax.axis_index("var")
    weight = jnp.float32(0.0)
    for index, value in enumerate(energy_weights):
        weight = jnp.where(variable == index, jnp.float32(value), weight)
    gap = jnp.zeros((8, LANES), jnp.float32)
    model = jnp.zeros((8, LANES), jnp.float32)
    for t in range(width // LANES):
        for r in range(0, modes, 8):
            at = (slice(r, r + 8), slice(t * LANES, (t + 1) * LANES))
            coeff = own_ref[at]
            for other in others:
                coeff = coeff + other[at]
            mask = mask_ref[at]
            delta = mask * (goal_ref[at] - coeff)
            delta_ref[at] = delta
            gap = gap + delta * delta
            model = model + mask * coeff * coeff
    gap = jnp.sum(gap, axis=0, keepdims=True)
    model = jnp.sum(model, axis=0, keepdims=True)
    energy_ref[...] = weight * jnp.where(lax.broadcasted_iota(jnp.int32, (8, LANES), 0) == 0, gap, model)


def inverse_kernel(which, delta_ref, lift_ref, tx_ref, ty_ref, out_ref):
    half, rows, _ = out_ref.shape
    modes, width = delta_ref.shape
    first = jnp.bitwise_xor(owned_half(), which) * half
    tiles = [delta_ref[:, t * LANES : (t + 1) * LANES] for t in range(width // LANES)]
    tall = jnp.concatenate(unpack_lanes(tiles, half, modes), axis=0)
    both = dot(stack_split(tall, 1), ty_ref[...])
    back = both[:, :LANES] + both[:, LANES:]
    wide = jnp.concatenate([back[l * modes : (l + 1) * modes] for l in range(half)], axis=1)
    both = dot(tx_ref[...], stack_split(wide, 0))
    for l in range(half):
        at = slice(l * LANES, (l + 1) * LANES)
        out_ref[l] = lift_ref[pl.ds(first + l, 1), :] * (both[:rows, at] + both[rows:, at])


def finish_kernel(energy_ref, last_ref, block_ref, own_ref, other_ref, out_ref, buffer, sems):
    half = own_ref.shape[0]
    core = owned_half()
    energy = energy_ref[...] + last_ref[...]
    gap = jnp.sum(energy[:1], keepdims=True)
    model = jnp.sum(energy[1:2], keepdims=True)
    strength = strength_top * gap / (gap + model + epsilon)
    count = sems.shape[0] // 2
    size = half // count
    copies = []
    for h, (ref, first) in enumerate(((own_ref, core * half), (other_ref, (1 - core) * half))):
        for q in range(count):
            for l in range(q * size, (q + 1) * size):
                buffer[h * half + l] = block_ref[first + l] + strength * ref[l]
            copies.append(
                pltpu.make_async_copy(
                    buffer.at[pl.ds(h * half + q * size, size)],
                    out_ref.at[0, pl.ds(first + q * size, size)],
                    sems.at[h * count + q],
                )
            )
            copies[-1].start()
    for copy in copies:
        copy.wait()


def call(kernel, ins, outs, scratch=(), flops=0):
    return pl.pallas_call(
        kernel,
        out_shape=outs,
        in_specs=[pl.BlockSpec(memory_space=pl.ANY if s is HBM else s) for _, s in ins],
        out_specs=jax.tree.map(
            lambda o: pl.BlockSpec(memory_space=VMEM if isinstance(o, pl.MemoryRef) else pl.ANY),
            outs,
            is_leaf=lambda o: isinstance(o, (pl.MemoryRef, jax.ShapeDtypeStruct)),
        ),
        scratch_shapes=scratch,
        cost_estimate=pl.CostEstimate(flops=flops, transcendentals=0, bytes_accessed=0),
    )(*[pltpu.with_memory_space_constraint(x, VMEM) if s is VMEM else x for x, s in ins])


def solution(mesh):
    count_x, count_y, count_v = (mesh.shape[a] for a in ("gx", "gy", "var"))
    ranks = count_x * count_y
    for count in (count_x, count_y, count_v):
        assert count & (count - 1) == 0

    def swap(value, bits, bits_v=0):
        bits = bits * count_v + bits_v
        pairs = [(i, i ^ bits) for i in range(ranks * count_v)]
        return lax.ppermute(value, ("gx", "gy", "var"), pairs)

    core = count_y

    bits_x = [count_y << b for b in range(1, count_x.bit_length() - 1)]
    bits_y = [1 << b for b in range(count_y.bit_length() - 1)]
    stages = []
    for b in range(max(len(bits_x), len(bits_y))):
        bx, by = bits_x[b : b + 1], bits_y[b : b + 1]
        stages.append([bits | core * ((bits + bits // (2 * core)) % 2) for bits in bx + by + [x | y for x in bx for y in by]])

    def nudge(field, drive, keep_count, level_class, height_table):
        _, levels, rows, columns = field.shape
        modes = drive.shape[-1]
        half = levels // 2
        total_x, total_y = rows * count_x, columns * count_y
        assert columns == LANES and levels % 4 == 0 and half * modes % LANES == 0 and modes % 8 == 0
        table_x = cosine_table(total_x, modes).reshape(count_x, rows, modes)
        table_y = np.zeros((count_y, columns, LANES), np.float32)
        table_y[:, :, :modes] = cosine_table(total_y, modes).reshape(count_y, columns, modes)
        tx_t = split_table(table_x.transpose(0, 2, 1) / np.float32(total_x * total_y), 2)
        ty = split_table(table_y, 1)
        tx = split_table(table_x, 2)
        ty_t = split_table(table_y.transpose(0, 2, 1), 1)
        packed = pltpu.VMEM((modes, half * modes), jnp.float32)
        cube = pltpu.VMEM((levels, rows, columns), jnp.float32)
        half_cube = pltpu.VMEM((half, rows, columns), jnp.float32)
        dma = pltpu.SemaphoreType.DMA
        like = lambda table: pltpu.VMEM(table.shape[1:], table.dtype)

        block, send, tx_t, ty = call(
            send_kernel,
            [(field, HBM), (jnp.asarray(tx_t), HBM), (jnp.asarray(ty), HBM)],
            (cube, packed, like(tx_t), like(ty)),
            [dma((4,))],
        )
        keep = call(keep_kernel, [(x, VMEM) for x in (block, tx_t, ty)], packed, flops=10**9)
        total = keep + swap(send, core)
        goal, mask, lift, tx, ty_t = call(
            prepare_kernel,
            [
                (total, VMEM),
                (keep_count, SMEM),
                (level_class, SMEM),
                (height_table, SMEM),
                (drive, HBM),
                (jnp.asarray(tx), HBM),
                (jnp.asarray(ty_t), HBM),
            ],
            (
                packed,
                packed,
                pltpu.VMEM((levels, LANES), jnp.float32),
                like(tx),
                like(ty_t),
            ),
            [pltpu.VMEM((half, modes, modes), jnp.float32), dma((3,))],
            flops=10**9,
        )
        parts = [total]
        for stage in stages:
            if len(parts) > 1:
                parts = [sum(parts[1:], parts[0])]
            parts = parts + [swap(parts[0], bits) for bits in stage]
        delta, energy = call(
            settle_kernel,
            [(x, VMEM) for x in (goal, mask, *parts)],
            (packed, pltpu.VMEM((8, LANES), jnp.float32)),
        )
        energy = energy + swap(energy, core)
        shared = swap(delta, core)
        own, other = (
            call(
                functools.partial(inverse_kernel, which),
                [(x, VMEM) for x in (part, lift, tx, ty_t)],
                half_cube,
                flops=10**9,
            )
            for which, part in ((0, delta), (1, shared))
        )
        last = jnp.zeros_like(energy)
        for b in range(count_v.bit_length() - 1):
            energy = energy + last
            last = swap(energy, core, 1 << b)
        return call(
            finish_kernel,
            [(x, VMEM) for x in (energy, last, block, own, other)],
            jax.ShapeDtypeStruct(field.shape, jnp.float32),
            [pltpu.VMEM((levels, rows, columns), jnp.float32), dma((4,))],
        )

    return jax.shard_map(
        nudge,
        mesh=mesh,
        in_specs=(P("var", None, "gx", "gy"), P("var", None, None, None), P(), P(), P()),
        out_specs=P("var", None, "gx", "gy"),
        check_vma=False,
    )
```

```python
import functools

import numpy as np

import jax
import jax.numpy as jnp
from jax import lax
from jax.experimental import pallas as pl
from jax.experimental.pallas import tpu as pltpu
from jax.sharding import PartitionSpec as P


energy_weights = (1.0, 1.0, 2.0, 3.0)
strength_top = 0.5
epsilon = 1e-06


LANES = 128
VMEM = pltpu.MemorySpace.VMEM
SMEM = pltpu.MemorySpace.SMEM
HBM = pltpu.MemorySpace.HBM


def cosine_table(total, modes):
    cells = np.arange(total, dtype=np.int64)
    waves = np.arange(modes, dtype=np.int64)
    phase = waves[None, :] * (2 * cells[:, None] + 1) % (4 * total)
    factor = np.where(waves == 0, 1.0, np.sqrt(2.0))
    return (np.cos(np.pi * phase / (2.0 * total)) * factor[None, :]).astype(np.float32)


def dot(a, b):
    return jnp.dot(a, b, preferred_element_type=jnp.float32)


def split(x):
    high = x.astype(jnp.bfloat16)
    return high, (x - high.astype(jnp.float32)).astype(jnp.bfloat16)


def stack_split(x, axis):
    return jnp.concatenate(split(x), axis=axis)


def split_table(table, axis):
    high = table.astype(jnp.bfloat16)
    low = (table - high.astype(np.float32)).astype(jnp.bfloat16)
    both = np.concatenate([high, low], axis=3 - axis)
    return np.concatenate([both, both], axis=axis)


def owned_half():
    at_x, at_y = lax.axis_index("gx"), lax.axis_index("gy")
    return lax.rem(at_x + at_x // 2 + at_y, 2)


def pack_lanes(pieces, modes):
    tiles = -(-len(pieces) * modes // LANES)
    out = [None] * tiles
    lane = lax.broadcasted_iota(jnp.int32, pieces[0].shape, 1)

    def put(tile, value):
        out[tile] = value if out[tile] is None else out[tile] + value

    for index, piece in enumerate(pieces):
        tile, offset = divmod(index * modes, LANES)
        turned = pltpu.roll(piece, offset, 1) if offset else piece
        if offset + modes > LANES:
            put(tile, jnp.where(lane >= offset, turned, 0.0))
            put(tile + 1, jnp.where(lane < offset, turned, 0.0))
        else:
            put(tile, turned)
    return out


def unpack_lanes(tiles, count, modes):
    lane = lax.broadcasted_iota(jnp.int32, tiles[0].shape, 1)
    pieces = []
    for index in range(count):
        tile, offset = divmod(index * modes, LANES)
        piece = tiles[tile]
        if offset + modes > LANES:
            piece = jnp.where(lane >= offset, piece, tiles[tile + 1])
        pieces.append(pltpu.roll(piece, LANES - offset, 1) if offset else piece)
    return pieces


def transform(block, tx, ty_ref, modes, ready=lambda: None):
    wide = stack_split(jnp.concatenate(block, axis=1), 0)
    both = dot(tx, wide)
    part = both[:modes] + both[modes:]
    tall = jnp.concatenate([part[:, l * LANES : (l + 1) * LANES] for l in range(len(block))], axis=0)
    ready()
    table = ty_ref[...]
    both = dot(stack_split(tall, 1), jnp.concatenate([table, table], axis=0))
    coeff = both[:, :LANES] + both[:, LANES:]
    return [coeff[l * modes : (l + 1) * modes] for l in range(len(block))]


def store_packed(out_ref, pieces, modes):
    for t, tile in enumerate(pack_lanes(pieces, modes)):
        out_ref[:, t * LANES : (t + 1) * LANES] = tile


def send_kernel(field_ref, tx_ref, ty_ref, block_ref, send_ref, tx, ty, sems):
    half = block_ref.shape[0] // 2
    modes = send_ref.shape[0]
    owned = owned_half()
    first = (1 - owned) * half

    def levels_copy(start, sem):
        rows = pl.ds(start, half)
        return pltpu.make_async_copy(field_ref.at[0, rows], block_ref.at[rows], sem)

    sent = levels_copy(first, sems.at[0])
    kept = levels_copy(owned * half, sems.at[1])
    tx_copy = pltpu.make_async_copy(tx_ref.at[lax.axis_index("gx")], tx, sems.at[2])
    ty_copy = pltpu.make_async_copy(ty_ref.at[lax.axis_index("gy")], ty, sems.at[3])
    for copy in (sent, tx_copy, ty_copy, kept):
        copy.start()
    tx_copy.wait()
    sent.wait()
    levels = [block_ref[first + l] for l in range(half)]
    store_packed(send_ref, transform(levels, tx[...], ty, modes, ty_copy.wait), modes)
    kept.wait()


def keep_kernel(block_ref, tx_ref, ty_ref, keep_ref):
    half = block_ref.shape[0] // 2
    modes = keep_ref.shape[0]
    first = owned_half() * half
    levels = [block_ref[first + l] for l in range(half)]
    store_packed(keep_ref, transform(levels, tx_ref[...], ty_ref, modes), modes)


def prepare_kernel(
    _,
    keep_count_ref,
    class_ref,
    height_ref,
    drive_ref,
    tx_ref,
    ty_ref,
    goal_ref,
    mask_ref,
    lift_ref,
    tx_out_ref,
    ty_out_ref,
    drive,
    sems,
):
    half, modes, _ = drive.shape
    width = goal_ref.shape[1]
    at_x, at_y = lax.axis_index("gx"), lax.axis_index("gy")
    first = owned_half() * half
    copies = [
        pltpu.make_async_copy(drive_ref.at[0, pl.ds(first, half)], drive, sems.at[0]),
        pltpu.make_async_copy(tx_ref.at[at_x], tx_out_ref, sems.at[1]),
        pltpu.make_async_copy(ty_ref.at[at_y], ty_out_ref, sems.at[2]),
    ]
    for copy in copies:
        copy.start()
    for l in range(lift_ref.shape[0]):
        lift_ref[l : l + 1, :] = jnp.full((1, LANES), height_ref[class_ref[l]], jnp.float32)
    lane = lax.broadcasted_iota(jnp.int32, (8, LANES), 1)
    row = lax.broadcasted_iota(jnp.int32, (8, LANES), 0)
    for t in range(width // LANES):
        limit = jnp.zeros((8, LANES), jnp.int32)
        for l in range(t * LANES // modes, min(half, ((t + 1) * LANES - 1) // modes + 1)):
            wave = lane + (t * LANES - l * modes)
            limit = jnp.where(wave >= 0, keep_count_ref[first + l] - wave, limit)
        for r in range(0, modes, 8):
            mask_ref[r : r + 8, t * LANES : (t + 1) * LANES] = (row + r < limit).astype(jnp.float32)
    copies[0].wait()
    pad = jnp.zeros((modes, LANES - modes), jnp.float32)
    goal = pack_lanes([jnp.concatenate([drive[l], pad], axis=1) for l in range(half)], modes)
    for t, tile in enumerate(goal):
        goal_ref[:, t * LANES : (t + 1) * LANES] = tile
    for copy in copies[1:]:
        copy.wait()


def settle_kernel(goal_ref, mask_ref, own_ref, *rest):
    *others, delta_ref, energy_ref = rest
    modes, width = own_ref.shape
    variable = lax.axis_index("var")
    weight = jnp.float32(0.0)
    for index, value in enumerate(energy_weights):
        weight = jnp.where(variable == index, jnp.float32(value), weight)
    gap = jnp.zeros((8, LANES), jnp.float32)
    model = jnp.zeros((8, LANES), jnp.float32)
    for t in range(width // LANES):
        for r in range(0, modes, 8):
            at = (slice(r, r + 8), slice(t * LANES, (t + 1) * LANES))
            coeff = own_ref[at]
            for other in others:
                coeff = coeff + other[at]
            mask = mask_ref[at]
            delta = mask * (goal_ref[at] - coeff)
            delta_ref[at] = delta
            gap = gap + delta * delta
            model = model + mask * coeff * coeff
    gap = jnp.sum(gap, axis=0, keepdims=True)
    model = jnp.sum(model, axis=0, keepdims=True)
    energy_ref[...] = weight * jnp.where(lax.broadcasted_iota(jnp.int32, (8, LANES), 0) == 0, gap, model)


def inverse_kernel(which, delta_ref, lift_ref, tx_ref, ty_ref, out_ref):
    half, rows, _ = out_ref.shape
    modes, width = delta_ref.shape
    first = jnp.bitwise_xor(owned_half(), which) * half
    tiles = [delta_ref[:, t * LANES : (t + 1) * LANES] for t in range(width // LANES)]
    tall = jnp.concatenate(unpack_lanes(tiles, half, modes), axis=0)
    both = dot(stack_split(tall, 1), ty_ref[...])
    back = both[:, :LANES] + both[:, LANES:]
    wide = jnp.concatenate([back[l * modes : (l + 1) * modes] for l in range(half)], axis=1)
    both = dot(tx_ref[...], stack_split(wide, 0))
    for l in range(half):
        at = slice(l * LANES, (l + 1) * LANES)
        out_ref[l] = lift_ref[pl.ds(first + l, 1), :] * (both[:rows, at] + both[rows:, at])


def finish_kernel(energy_ref, last_ref, block_ref, own_ref, other_ref, out_ref, buffer, sems):
    half = own_ref.shape[0]
    core = owned_half()
    energy = energy_ref[...] + last_ref[...]
    total = jnp.sum(energy, axis=1, keepdims=True)
    gap, model = total[:1], total[1:2]
    strength = strength_top * gap / (gap + model + epsilon)
    count = sems.shape[0] // 2
    size = half // count
    copies = []
    for h, (ref, first) in enumerate(((own_ref, core * half), (other_ref, (1 - core) * half))):
        for q in range(count):
            for l in range(q * size, (q + 1) * size):
                buffer[h * half + l] = block_ref[first + l] + strength * ref[l]
            copies.append(
                pltpu.make_async_copy(
                    buffer.at[pl.ds(h * half + q * size, size)],
                    out_ref.at[0, pl.ds(first + q * size, size)],
                    sems.at[h * count + q],
                )
            )
            copies[-1].start(priority=q % 2)
    for copy in copies:
        copy.wait()


def call(kernel, ins, outs, scratch=(), flops=0):
    return pl.pallas_call(
        kernel,
        out_shape=outs,
        in_specs=[pl.BlockSpec(memory_space=pl.ANY if s is HBM else s) for _, s in ins],
        out_specs=jax.tree.map(
            lambda o: pl.BlockSpec(memory_space=VMEM if isinstance(o, pl.MemoryRef) else pl.ANY),
            outs,
            is_leaf=lambda o: isinstance(o, (pl.MemoryRef, jax.ShapeDtypeStruct)),
        ),
        scratch_shapes=scratch,
        cost_estimate=pl.CostEstimate(flops=flops, transcendentals=0, bytes_accessed=0),
    )(*[pltpu.with_memory_space_constraint(x, VMEM) if s is VMEM else x for x, s in ins])


def solution(mesh):
    count_x, count_y, count_v = (mesh.shape[a] for a in ("gx", "gy", "var"))
    ranks = count_x * count_y
    for count in (count_x, count_y, count_v):
        assert count & (count - 1) == 0

    def swap(value, bits, bits_v=0):
        bits = bits * count_v + bits_v
        pairs = [(i, i ^ bits) for i in range(ranks * count_v)]
        return lax.ppermute(value, ("gx", "gy", "var"), pairs)

    core = count_y

    bits_x = [count_y << b for b in range(1, count_x.bit_length() - 1)]
    bits_y = [1 << b for b in range(count_y.bit_length() - 1)]
    stages = []
    for b in range(max(len(bits_x), len(bits_y))):
        bx, by = bits_x[b : b + 1], bits_y[b : b + 1]
        stages.append([bits | core * ((bits + bits // (2 * core)) % 2) for bits in bx + by + [x | y for x in bx for y in by]])

    def nudge(field, drive, keep_count, level_class, height_table):
        _, levels, rows, columns = field.shape
        modes = drive.shape[-1]
        half = levels // 2
        total_x, total_y = rows * count_x, columns * count_y
        assert columns == LANES and levels % 4 == 0 and half * modes % LANES == 0 and modes % 8 == 0
        table_x = cosine_table(total_x, modes).reshape(count_x, rows, modes)
        table_y = np.zeros((count_y, columns, LANES), np.float32)
        table_y[:, :, :modes] = cosine_table(total_y, modes).reshape(count_y, columns, modes)
        tx_t = split_table(table_x.transpose(0, 2, 1) / np.float32(total_x * total_y), 2)
        ty = split_table(table_y, 1)[:, :columns]
        tx = split_table(table_x, 2)
        ty_t = split_table(table_y.transpose(0, 2, 1), 1)
        packed = pltpu.VMEM((modes, half * modes), jnp.float32)
        cube = pltpu.VMEM((levels, rows, columns), jnp.float32)
        half_cube = pltpu.VMEM((half, rows, columns), jnp.float32)
        dma = pltpu.SemaphoreType.DMA
        like = lambda table: pltpu.VMEM(table.shape[1:], table.dtype)

        block, send, tx_t, ty = call(
            send_kernel,
            [(field, HBM), (jnp.asarray(tx_t), HBM), (jnp.asarray(ty), HBM)],
            (cube, packed, like(tx_t), like(ty)),
            [dma((4,))],
        )
        keep = call(keep_kernel, [(x, VMEM) for x in (block, tx_t, ty)], packed, flops=10**9)
        total = keep + swap(send, core)
        goal, mask, lift, tx, ty_t = call(
            prepare_kernel,
            [
                (total, VMEM),
                (keep_count, SMEM),
                (level_class, SMEM),
                (height_table, SMEM),
                (drive, HBM),
                (jnp.asarray(tx), HBM),
                (jnp.asarray(ty_t), HBM),
            ],
            (
                packed,
                packed,
                pltpu.VMEM((levels, LANES), jnp.float32),
                like(tx),
                like(ty_t),
            ),
            [pltpu.VMEM((half, modes, modes), jnp.float32), dma((3,))],
            flops=10**9,
        )
        parts = [total]
        for stage in stages:
            if len(parts) > 1:
                parts = [sum(parts[1:], parts[0])]
            parts = parts + [swap(parts[0], bits) for bits in stage]
        delta, energy = call(
            settle_kernel,
            [(x, VMEM) for x in (goal, mask, *parts)],
            (packed, pltpu.VMEM((8, LANES), jnp.float32)),
        )
        energy = energy + swap(energy, core)
        shared = swap(delta, core)
        own, other = (
            call(
                functools.partial(inverse_kernel, which),
                [(x, VMEM) for x in (part, lift, tx, ty_t)],
                half_cube,
                flops=10**9,
            )
            for which, part in ((0, delta), (1, shared))
        )
        last = jnp.zeros_like(energy)
        for b in range(count_v.bit_length() - 1):
            energy = energy + last
            last = swap(energy, core, 1 << b)
        return call(
            finish_kernel,
            [(x, VMEM) for x in (energy, last, block, own, other)],
            jax.ShapeDtypeStruct(field.shape, jnp.float32),
            [pltpu.VMEM((levels, rows, columns), jnp.float32), dma((4,))],
        )

    return jax.shard_map(
        nudge,
        mesh=mesh,
        in_specs=(P("var", None, "gx", "gy"), P("var", None, None, None), P(), P(), P()),
        out_specs=P("var", None, "gx", "gy"),
        check_vma=False,
    )
```
